32 devices in a mesh: dp: 8 (over y, x, core), seq: 4 (over z).
Axes of the slice: x: 2, y: 2, z: 4, core: 2. Of those that a mesh axis runs over, the one named last changes fastest.
Arguments:
- layer_input: bfloat16 [8, 512, 2048], P('dp', 'seq'), may hold values from -6 to 6
- cotangent: bfloat16 [8, 512, 2048], P('dp', 'seq'), may hold values from -6 to 6
- ln1_gain: float32 [2048], P('dp'), may hold values from 0.5 to 1.5
- ln1_bias: float32 [2048], P('dp'), may hold values from -3 to 3
- w_qkv: bfloat16 [2048, 6144], P('dp'), may hold values from -0.125 to 0.125
- b_qkv: float32 [6144], P('dp'), may hold values from -3 to 3
- w_out: bfloat16 [2048, 2048], P('dp'), may hold values from -0.5 to 0.5
- b_out: float32 [2048], P('dp'), may hold values from -3 to 3
- ln2_gain: float32 [2048], P('dp'), may hold values from 0.5 to 1.5
- ln2_bias: float32 [2048], P('dp'), may hold values from -3 to 3
- w_up: bfloat16 [2048, 8192], P('dp'), may hold values from -0.125 to 0.125
- b_up: float32 [8192], P('dp'), may hold values from -3 to 3
- w_down: bfloat16 [8192, 2048], P('dp'), may hold values from -0.0625 to 0.0625
- b_down: float32 [2048], P('dp'), may hold values from -3 to 3
Outputs:
- output: float32 [8, 512, 2048], P('dp', 'seq')
- input_grad: float32 [8, 512, 2048], P('dp', 'seq')
- ln1_gain_grad: float32 [2048], P('dp')
- ln1_bias_grad: float32 [2048], P('dp')
- w_qkv_grad: float32 [2048, 6144], P('dp')
- b_qkv_grad: float32 [6144], P('dp')
- w_out_grad: float32 [2048, 2048], P('dp')
- b_out_grad: float32 [2048], P('dp')
- ln2_gain_grad: float32 [2048], P('dp')
- ln2_bias_grad: float32 [2048], P('dp')
- w_up_grad: float32 [2048, 8192], P('dp')
- b_up_grad: float32 [8192], P('dp')
- w_down_grad: float32 [8192, 2048], P('dp')
- b_down_grad: float32 [2048], P('dp')
The draws below stay inside these ranges and needn't reach their ends.
All inputs are finite; a program needn't handle non-finite values.
Results may differ from the reference program's by a relative error of at most 0.029.
Values may be sent and summed in bfloat16 or wider, within the bound.
A program may use at most 640 MiB of HBM per device.

```python
import jax
import jax.numpy as jnp
from jax import lax

D = 2048
H = 8
HD = 256
FF = 8192
ROT = 64
SEQ_LEN = 512
BATCH = 8


def steps_of(rng, dims, shards, least, top_value):
    level = 1.0
    for axis_at, parts in shards:
        draws = jax.random.uniform(jax.random.fold_in(jax.random.fold_in(rng, 6), axis_at), (parts,), jnp.float32, least / len(shards), top_value / len(shards))
        level = level * jnp.repeat(jnp.exp(draws), dims[axis_at] // parts).reshape((-1,) + (1,) * (len(dims) - 1 - axis_at))
    return level


def gaussian(rng, shape, deviation, bound, pieces=(), held_as=jnp.bfloat16):
    result = deviation * jax.random.normal(rng, shape, jnp.float32)
    if pieces:
        result = result * steps_of(rng, shape, pieces, -0.22, 0.18)
    return jnp.clip(result, -bound, bound).astype(held_as)


def setup_inputs(seed: int = 0) -> dict:
    keys = jax.random.split(jax.random.key(seed), 15)
    layer_input = gaussian(keys[0], (BATCH, SEQ_LEN, D), 1.0, 6.0, ((0, 8), (1, 4)))
    cotangent = gaussian(keys[1], (BATCH, SEQ_LEN, D), 1.0, 6.0, ((0, 8), (1, 4)))
    ln1_gain = jnp.clip(1.0 + 0.1 * jax.random.normal(keys[2], (D,), jnp.float32), 0.5, 1.5)
    ln1_bias = gaussian(keys[3], (D,), 0.3, 3.0, ((0, 8),), jnp.float32)
    w_qkv = gaussian(keys[4], (D, 3 * D), D ** -0.5, 0.125, ((0, 8),))
    b_qkv = gaussian(keys[5], (3 * D,), 0.5, 3.0, ((0, 8),), jnp.float32)
    w_out = gaussian(keys[6], (D, D), (D // 16) ** -0.5, 0.5, ((0, 8),))
    b_out = gaussian(keys[7], (D,), 0.3, 3.0, ((0, 8),), jnp.float32)
    ln2_gain = jnp.clip(1.0 + 0.1 * jax.random.normal(keys[8], (D,), jnp.float32), 0.5, 1.5)
    ln2_bias = gaussian(keys[9], (D,), 0.3, 3.0, ((0, 8),), jnp.float32)
    w_up = gaussian(keys[10], (D, FF), D ** -0.5, 0.125, ((0, 8),))
    b_up = gaussian(keys[11], (FF,), 0.5, 3.0, ((0, 8),), jnp.float32)
    w_down = gaussian(keys[12], (FF, D), FF ** -0.5, 0.0625, ((0, 8),))
    b_down = gaussian(keys[13], (D,), 1.0, 3.0, ((0, 8),), jnp.float32)
    return {"layer_input": layer_input, "cotangent": cotangent, "ln1_gain": ln1_gain, "ln1_bias": ln1_bias, "w_qkv": w_qkv, "b_qkv": b_qkv, "w_out": w_out, "b_out": b_out, "ln2_gain": ln2_gain, "ln2_bias": ln2_bias, "w_up": w_up, "b_up": b_up, "w_down": w_down, "b_down": b_down}


epsilon = 1e-05
masked_fill = -1e+30

def normalize(rows, gain, shift):
    center = rows - lax.optimization_barrier(jnp.mean(rows, axis=-1, keepdims=True))
    factor = lax.rsqrt(lax.optimization_barrier(jnp.mean(center * center, axis=-1, keepdims=True)) + epsilon)
    normed = center * factor
    return (normed, factor, normed * gain + shift)

def normalize_back(incoming, normed, factor, gain):
    scaled = incoming * gain
    return factor * (scaled - lax.optimization_barrier(jnp.mean(scaled, axis=-1, keepdims=True)) - normed * lax.optimization_barrier(jnp.mean(scaled * normed, axis=-1, keepdims=True)))

def gelu_value(inner):
    return inner * 0.5 * (1.0 + jax.scipy.special.erf(inner * 0.7071067811865476))

def gelu_slope(inner):
    cumulative = 0.5 * (1.0 + jax.scipy.special.erf(inner * 0.7071067811865476))
    return cumulative + inner * jnp.exp(-0.5 * inner * inner) * 0.3989422804014327

def angles(positions):
    half = ROT // 2
    freqs = 10000.0 ** (-2.0 * jnp.arange(half).astype(positions.dtype) / ROT)
    theta = positions[:, None] * freqs[None, :]
    return (jnp.cos(theta), jnp.sin(theta))

def rotate(tensor, cosine, sine, direction):
    half = ROT // 2
    first_half = tensor[..., :half]
    second_half = tensor[..., half:ROT]
    return jnp.concatenate([first_half * cosine - direction * second_half * sine, second_half * cosine + direction * first_half * sine, tensor[..., ROT:]], axis=-1)

def masked_scores(queries, key_rows):
    scores = jnp.dot(queries, key_rows.T, preferred_element_type=jnp.float32) * HD ** (-0.5)
    allowed = jnp.arange(SEQ_LEN)[None, :] <= jnp.arange(SEQ_LEN)[:, None]
    return jnp.where(allowed, scores, masked_fill)

def head_forward(queries, key_rows, values):
    scores = masked_scores(queries, key_rows)
    top = lax.optimization_barrier(jnp.max(scores, axis=-1, keepdims=True))
    logsum = top[:, 0] + jnp.log(lax.optimization_barrier(jnp.sum(jnp.exp(scores - top), axis=-1)))
    probs = jnp.exp(scores - logsum[:, None]).astype(jnp.bfloat16)
    context = jnp.dot(probs, values, preferred_element_type=jnp.float32).astype(jnp.bfloat16)
    return (context, logsum)

def head_backward(queries, key_rows, values, context, logsum, incoming):
    scores = masked_scores(queries, key_rows)
    probs_f = jnp.exp(scores - logsum[:, None])
    probs = probs_f.astype(jnp.bfloat16)
    value_grad = jnp.dot(probs.T, incoming, preferred_element_type=jnp.float32).astype(jnp.bfloat16)
    prob_grad = jnp.dot(incoming, values.T, preferred_element_type=jnp.float32)
    delta = lax.optimization_barrier(jnp.sum(incoming.astype(jnp.float32) * context.astype(jnp.float32), axis=-1))
    score_grad = (probs_f * (prob_grad - delta[:, None]) * HD ** (-0.5)).astype(jnp.bfloat16)
    query_grad = jnp.dot(score_grad, key_rows, preferred_element_type=jnp.float32).astype(jnp.bfloat16)
    key_grad = jnp.dot(score_grad.T, queries, preferred_element_type=jnp.float32).astype(jnp.bfloat16)
    return (query_grad, key_grad, value_grad)

def heads_first(tensor):
    return jnp.transpose(tensor, (1, 0, 2))

def reference(layer_input, cotangent, ln1_gain, ln1_bias, w_qkv, b_qkv, w_out, b_out, ln2_gain, ln2_bias, w_up, b_up, w_down, b_down):
    cosine, sine = angles(jnp.arange(SEQ_LEN).astype(ln1_gain.dtype))
    cosine = cosine[:, None, :]
    sine = sine[:, None, :]

    def one_sequence(totals, pair):
        tokens, incoming = pair
        rows = tokens.astype(jnp.float32)
        normed_one, factor_one, attn_in = normalize(rows, ln1_gain, ln1_bias)
        attn_in = attn_in.astype(jnp.bfloat16)
        triple = (jnp.dot(attn_in, w_qkv, preferred_element_type=jnp.float32) + b_qkv).reshape(SEQ_LEN, 3, H, HD)
        queries = rotate(triple[:, 0], cosine, sine, 1.0).astype(jnp.bfloat16)
        key_rows = rotate(triple[:, 1], cosine, sine, 1.0).astype(jnp.bfloat16)
        values = triple[:, 2].astype(jnp.bfloat16)
        query_heads = heads_first(queries)
        key_heads = heads_first(key_rows)
        value_heads = heads_first(values)
        context, logsum = lax.map(lambda item: head_forward(item[0], item[1], item[2]), (query_heads, key_heads, value_heads))
        merged = heads_first(context).reshape(SEQ_LEN, D)
        attended = jnp.dot(merged, w_out, preferred_element_type=jnp.float32) + b_out
        normed_two, factor_two, mlp_in = normalize(rows, ln2_gain, ln2_bias)
        mlp_in = mlp_in.astype(jnp.bfloat16)
        inner = jnp.dot(mlp_in, w_up, preferred_element_type=jnp.float32) + b_up
        hidden = gelu_value(inner).astype(jnp.bfloat16)
        output = rows + attended + jnp.dot(hidden, w_down, preferred_element_type=jnp.float32) + b_down
        grad_rows = incoming.astype(jnp.float32)
        w_down_grad = jnp.dot(hidden.T, incoming, preferred_element_type=jnp.float32)
        b_down_grad = lax.optimization_barrier(jnp.sum(grad_rows, axis=0))
        inner_grad = jnp.dot(incoming, w_down.T, preferred_element_type=jnp.float32) * gelu_slope(inner)
        inner_grad_b = inner_grad.astype(jnp.bfloat16)
        w_up_grad = jnp.dot(mlp_in.T, inner_grad_b, preferred_element_type=jnp.float32)
        b_up_grad = lax.optimization_barrier(jnp.sum(inner_grad, axis=0))
        mlp_in_grad = jnp.dot(inner_grad_b, w_up.T, preferred_element_type=jnp.float32)
        ln2_gain_grad = lax.optimization_barrier(jnp.sum(mlp_in_grad * normed_two, axis=0))
        ln2_bias_grad = lax.optimization_barrier(jnp.sum(mlp_in_grad, axis=0))
        w_out_grad = jnp.dot(merged.T, incoming, preferred_element_type=jnp.float32)
        b_out_grad = lax.optimization_barrier(jnp.sum(grad_rows, axis=0))
        context_grad = jnp.dot(incoming, w_out.T, preferred_element_type=jnp.float32).astype(jnp.bfloat16).reshape(SEQ_LEN, H, HD)
        query_grad, key_grad, value_grad = lax.map(lambda item: head_backward(item[0], item[1], item[2], item[3], item[4], item[5]), (query_heads, key_heads, value_heads, context, logsum, heads_first(context_grad)))
        query_back = rotate(heads_first(query_grad).astype(jnp.float32), cosine, sine, -1.0)
        key_back = rotate(heads_first(key_grad).astype(jnp.float32), cosine, sine, -1.0)
        triple_grad = jnp.stack([query_back, key_back, heads_first(value_grad).astype(jnp.float32)], axis=1).reshape(SEQ_LEN, 3 * D)
        triple_grad_b = triple_grad.astype(jnp.bfloat16)
        w_qkv_grad = jnp.dot(attn_in.T, triple_grad_b, preferred_element_type=jnp.float32)
        b_qkv_grad = lax.optimization_barrier(jnp.sum(triple_grad, axis=0))
        attn_in_grad = jnp.dot(triple_grad_b, w_qkv.T, preferred_element_type=jnp.float32)
        ln1_gain_grad = lax.optimization_barrier(jnp.sum(attn_in_grad * normed_one, axis=0))
        ln1_bias_grad = lax.optimization_barrier(jnp.sum(attn_in_grad, axis=0))
        grad_input = grad_rows + normalize_back(attn_in_grad, normed_one, factor_one, ln1_gain) + normalize_back(mlp_in_grad, normed_two, factor_two, ln2_gain)
        terms = (ln1_gain_grad, ln1_bias_grad, w_qkv_grad, b_qkv_grad, w_out_grad, b_out_grad, ln2_gain_grad, ln2_bias_grad, w_up_grad, b_up_grad, w_down_grad, b_down_grad)
        totals = tuple((total + term for total, term in zip(totals, terms)))
        return (totals, (output, grad_input))
    shapes = (ln1_gain, ln1_bias, w_qkv, b_qkv, w_out, b_out, ln2_gain, ln2_bias, w_up, b_up, w_down, b_down)
    zeros = tuple((jnp.zeros(item.shape, ln1_gain.dtype) for item in shapes))
    totals, stacked = lax.scan(one_sequence, zeros, (layer_input, cotangent))
    return (stacked[0], stacked[1], totals[0], totals[1], totals[2], totals[3], totals[4], totals[5], totals[6], totals[7], totals[8], totals[9], totals[10], totals[11])
```

```python
import jax
import jax.numpy as jnp
from jax import lax
from jax.sharding import PartitionSpec as P

H = 8
HD = 256
ROT = 64

epsilon = 1e-05
masked_fill = -1e30


def dot(a, b, contract):
    return lax.dot_general(a, b, (contract, ((), ())), preferred_element_type=jnp.float32)


def normalize(rows):
    center = rows - jnp.mean(rows, axis=-1, keepdims=True)
    factor = lax.rsqrt(jnp.mean(center * center, axis=-1, keepdims=True) + epsilon)
    return center * factor, factor


def angles(positions):
    half = ROT // 2
    freqs = 10000.0 ** (-2.0 * jnp.arange(half).astype(positions.dtype) / ROT)
    theta = positions[:, None] * freqs[None, :]
    return (jnp.cos(theta), jnp.sin(theta))


def rotate(tensor, cosine, sine, direction):
    half = ROT // 2
    first_half = tensor[..., :half]
    second_half = tensor[..., half:ROT]
    return jnp.concatenate(
        [
            first_half * cosine - direction * second_half * sine,
            second_half * cosine + direction * first_half * sine,
            tensor[..., ROT:],
        ],
        axis=-1,
    )


def gather_dp(rows):
    return lax.all_gather(rows, "dp", axis=0, tiled=True)


def gather_seq(shard):
    return lax.all_gather(shard, "seq", axis=0, tiled=False)


def scatter_dp(rows):
    return lax.psum_scatter(rows, "dp", scatter_dimension=0, tiled=True)


def exchange_sum(partial, n_seq):
    slabs = partial.astype(jnp.bfloat16).reshape(n_seq, partial.shape[0] // n_seq, partial.shape[1])
    got = lax.all_to_all(slabs, "seq", split_axis=0, concat_axis=0, tiled=True)
    return jnp.sum(got.astype(jnp.float32), axis=0)


def make_local(n_dp, n_seq):
    def local(
        layer_input,
        cotangent,
        ln1_gain,
        ln1_bias,
        w_qkv,
        b_qkv,
        w_out,
        b_out,
        ln2_gain,
        ln2_bias,
        w_up,
        b_up,
        w_down,
        b_down,
    ):
        f32, bf16 = jnp.float32, jnp.bfloat16
        _, tok_local, width = layer_input.shape
        length = tok_local * n_seq
        own = width // n_dp
        ff = w_up.shape[1]
        ff_own = ff // n_dp
        unit = ff_own // n_seq
        heads = H // n_seq
        z = lax.axis_index("seq")

        up_own = lax.dynamic_index_in_dim(
            w_up.reshape(own, n_dp, n_seq, unit), z, 2, keepdims=False
        ).reshape(own, n_dp * unit)
        up_w = gather_dp(up_own)
        down_own = lax.dynamic_slice_in_dim(w_down, z * unit, unit, 0)
        down_w = gather_dp(down_own)
        qkv_own = lax.dynamic_slice_in_dim(
            w_qkv.reshape(own, 3, H, HD), z * heads, heads, 2
        ).reshape(own, 3 * heads * HD)
        triple_w = gather_dp(qkv_own)
        owners = n_dp // n_seq
        piece = own // n_dp
        spread = lax.all_to_all(
            w_out.reshape(n_dp, piece, width), "dp", split_axis=0, concat_axis=0, tiled=True
        )
        out_own = lax.dynamic_slice_in_dim(spread, z * owners, owners, 0)
        out_w = (
            lax.all_gather(out_own, "dp", axis=0, tiled=False)
            .transpose(1, 0, 2, 3)
            .reshape(owners * own, width)
        )

        packed = jnp.concatenate(
            [ln1_gain, ln1_bias, ln2_gain, ln2_bias, b_out, b_down, b_qkv, b_up]
        )
        gathered = lax.all_gather(packed, "dp", axis=0, tiled=False)
        gain_one, shift_one, gain_two, shift_two, out_b, down_b = (
            gathered[:, k * own : (k + 1) * own].reshape(width) for k in range(6)
        )
        base = 6 * own
        triple_b = lax.dynamic_slice_in_dim(
            gathered[:, base : base + 3 * own].reshape(3, H, HD), z * heads, heads, 1
        ).reshape(3 * heads * HD)
        up_b = lax.dynamic_index_in_dim(
            gathered[:, base + 3 * own :].reshape(n_dp, n_seq, unit), z, 1, keepdims=False
        ).reshape(n_dp * unit)

        tokens = gather_seq(layer_input.reshape(tok_local, width)).reshape(length, width)
        incoming = gather_seq(cotangent.reshape(tok_local, width)).reshape(length, width)

        normed, _ = normalize(tokens.astype(f32))
        mlp_in = (normed * gain_two + shift_two).astype(bf16)
        attn_in = (normed * gain_one + shift_one).astype(bf16)

        inner = dot(mlp_in, up_w, ((1,), (0,))) + up_b
        cumulative = 0.5 * (1.0 + lax.erf(inner * 0.7071067811865476))
        hidden = (inner * cumulative).astype(bf16)
        slope = cumulative + inner * jnp.exp(-0.5 * inner * inner) * 0.3989422804014327
        down_grad = dot(hidden, incoming, ((0,), (0,))).astype(bf16)
        inner_grad = dot(incoming, down_w, ((1,), (1,))) * slope
        inner_grad_b = inner_grad.astype(bf16)
        up_grad = dot(mlp_in, inner_grad_b, ((0,), (0,))).astype(bf16)
        mlp_out = dot(hidden, down_w, ((1,), (0,)))
        mlp_in_grad = dot(inner_grad_b, up_w, ((1,), (1,)))
        b_up_grad = jnp.sum(inner_grad, axis=0)
        ln2_gain_grad = jnp.sum(mlp_in_grad * normed, axis=0)
        ln2_bias_grad = jnp.sum(mlp_in_grad, axis=0)

        cosine, sine = angles(jnp.arange(length, dtype=jnp.int32).astype(f32))
        cosine, sine = cosine[:, None, :], sine[:, None, :]
        triple = (dot(attn_in, triple_w, ((1,), (0,))) + triple_b).reshape(length, 3, heads, HD)
        queries = rotate(triple[:, 0], cosine, sine, 1.0).astype(bf16)
        key_rows = rotate(triple[:, 1], cosine, sine, 1.0).astype(bf16)
        values = triple[:, 2].astype(bf16)
        scores = jnp.einsum("qhd,khd->hqk", queries, key_rows, preferred_element_type=f32) * HD ** (
            -0.5
        )
        order = jnp.arange(length, dtype=jnp.int32)
        scores = jnp.where((order[None, :] <= order[:, None])[None], scores, masked_fill)
        top = jnp.max(scores, axis=-1, keepdims=True)
        logsum = top + jnp.log(jnp.sum(jnp.exp(scores - top), axis=-1, keepdims=True))
        probs_f = jnp.exp(scores - logsum)
        probs = probs_f.astype(bf16)
        context = jnp.einsum("hqk,khd->qhd", probs, values, preferred_element_type=f32).astype(bf16)
        merged = context.reshape(length, heads * HD)
        attended = dot(merged, out_w, ((1,), (0,)))
        out_grad = dot(merged, incoming, ((0,), (0,))).astype(bf16)
        context_grad = dot(incoming, out_w, ((1,), (1,))).astype(bf16).reshape(length, heads, HD)
        delta = jnp.sum(context_grad.astype(f32) * context.astype(f32), axis=-1)
        value_grad = jnp.einsum(
            "hqk,qhd->khd", probs, context_grad, preferred_element_type=f32
        ).astype(bf16)
        prob_grad = jnp.einsum("qhd,khd->hqk", context_grad, values, preferred_element_type=f32)
        score_grad = (probs_f * (prob_grad - delta.T[:, :, None]) * HD ** (-0.5)).astype(bf16)
        query_grad = jnp.einsum(
            "hqk,khd->qhd", score_grad, key_rows, preferred_element_type=f32
        ).astype(bf16)
        key_grad = jnp.einsum(
            "hqk,qhd->khd", score_grad, queries, preferred_element_type=f32
        ).astype(bf16)
        triple_grad = jnp.stack(
            [
                rotate(query_grad.astype(f32), cosine, sine, -1.0),
                rotate(key_grad.astype(f32), cosine, sine, -1.0),
                value_grad.astype(f32),
            ],
            axis=1,
        ).reshape(length, 3 * heads * HD)
        triple_grad_b = triple_grad.astype(bf16)
        b_qkv_grad = jnp.sum(triple_grad, axis=0)
        qkv_grad = dot(attn_in, triple_grad_b, ((0,), (0,))).astype(bf16)
        attn_in_grad = dot(triple_grad_b, triple_w, ((1,), (1,)))
        ln1_gain_grad = jnp.sum(attn_in_grad * normed, axis=0)
        ln1_bias_grad = jnp.sum(attn_in_grad, axis=0)

        rows = layer_input.reshape(tok_local, width).astype(f32)
        grad_rows = cotangent.reshape(tok_local, width).astype(f32)
        output = rows + (out_b + down_b) + exchange_sum(attended + mlp_out, n_seq)
        scaled = exchange_sum(attn_in_grad * gain_one + mlp_in_grad * gain_two, n_seq)
        normed_own, factor_own = normalize(rows)
        input_grad = grad_rows + factor_own * (
            scaled
            - jnp.mean(scaled, axis=-1, keepdims=True)
            - normed_own * jnp.mean(scaled * normed_own, axis=-1, keepdims=True)
        )

        down_part = gather_seq(scatter_dp(down_grad))
        down_full = down_part.reshape(ff_own, width).astype(f32)
        up_part = gather_seq(scatter_dp(up_grad))
        up_full = (
            up_part.reshape(n_seq, own, n_dp, unit).transpose(1, 2, 0, 3).reshape(own, ff)
        ).astype(f32)
        out_part = gather_seq(
            scatter_dp(
                out_grad.reshape(owners, n_dp, piece, width)
                .transpose(1, 0, 2, 3)
                .reshape(n_dp * owners * piece, width)
            )
        )
        out_full = (
            lax.all_to_all(
                out_part.reshape(n_dp, piece, width), "dp", split_axis=0, concat_axis=0, tiled=True
            )
            .reshape(own, width)
            .astype(f32)
        )
        qkv_part = gather_seq(scatter_dp(qkv_grad))
        qkv_full = (
            qkv_part.reshape(n_seq, own, 3, heads * HD)
            .transpose(1, 2, 0, 3)
            .reshape(own, 3 * width)
            .astype(f32)
        )

        here = jnp.arange(n_seq) == z
        b_up_wide = jnp.where(
            here[None, :, None], b_up_grad.reshape(n_dp, 1, unit), 0.0
        ).reshape(n_dp, ff_own)
        b_qkv_wide = jnp.where(
            here[None, :, None], b_qkv_grad.reshape(3, 1, heads * HD), 0.0
        ).reshape(n_dp, 3 * own)
        b_down_grad = jnp.sum(grad_rows, axis=0)
        small = jnp.concatenate(
            [
                ln1_gain_grad.reshape(n_dp, own),
                ln1_bias_grad.reshape(n_dp, own),
                ln2_gain_grad.reshape(n_dp, own),
                ln2_bias_grad.reshape(n_dp, own),
                b_down_grad.reshape(n_dp, own),
                b_qkv_wide,
                b_up_wide,
            ],
            axis=1,
        )
        small = lax.psum(small, ("dp", "seq"))
        mine = lax.dynamic_index_in_dim(small, lax.axis_index("dp"), 0, keepdims=False)
        g1, s1, g2, s2, bd = (mine[k * own : (k + 1) * own] for k in range(5))
        bq = mine[5 * own : 8 * own]
        bu = mine[8 * own :]

        return (
            output.reshape(layer_input.shape),
            input_grad.reshape(layer_input.shape),
            g1,
            s1,
            qkv_full,
            bq,
            out_full,
            bd,
            g2,
            s2,
            up_full,
            bu,
            down_full,
            bd,
        )

    return local


def solution(mesh):
    vector, matrix, tokens = P("dp"), P("dp", None), P("dp", "seq", None)
    in_specs = (
        tokens,
        tokens,
        vector,
        vector,
        matrix,
        vector,
        matrix,
        vector,
        vector,
        vector,
        matrix,
        vector,
        matrix,
        vector,
    )
    out_specs = (
        tokens,
        tokens,
        vector,
        vector,
        matrix,
        vector,
        matrix,
        vector,
        vector,
        vector,
        matrix,
        vector,
        matrix,
        vector,
    )
    local = make_local(mesh.shape["dp"], mesh.shape["seq"])
    return jax.shard_map(
        local, mesh=mesh, in_specs=in_specs, out_specs=out_specs, check_vma=False
    )
```

```python
import functools

import jax
import jax.numpy as jnp
from jax import lax
from jax.experimental import pallas as pl
from jax.experimental.pallas import tpu as pltpu
from jax.sharding import PartitionSpec as P

H = 8
HD = 256
ROT = 64

epsilon = 1e-05
masked_fill = -1e30

MESH = pl.DeviceIdType.MESH


def bits_of(n):
    return n.bit_length() - 1


def flipped(me, mask):
    for k in range(mask.bit_length()):
        if mask >> k & 1:
            me = me + (1 << k) * (1 - 2 * ((me // (1 << k)) % 2))
    return me


def chip_orders(n):
    chips = [1 << k for k in range(1, bits_of(n))]
    return chips, chips[1:] + chips[:1]


def greet(n_dp, n_seq, me, z, along_seq):
    barrier = pltpu.get_barrier_semaphore()
    peers = bits_of(n_dp)
    for k in range(bits_of(n_dp)):
        pl.semaphore_signal(
            barrier, inc=1, device_id={"dp": flipped(me, 1 << k)}, device_id_type=MESH
        )
    if along_seq:

        @pl.when(z > 0)
        def _():
            pl.semaphore_signal(barrier, inc=1, device_id={"seq": z - 1}, device_id_type=MESH)

        @pl.when(z < n_seq - 1)
        def _():
            pl.semaphore_signal(barrier, inc=1, device_id={"seq": z + 1}, device_id_type=MESH)

        peers = peers + (z + n_seq - 1) // n_seq + (2 * n_seq - 2 - z) // n_seq
    pl.semaphore_wait(barrier, peers)


class Spread:
    def __init__(self, n_dp, me, own, out, send_sem, recv_sem):
        self.n_dp, self.me, self.own, self.out = n_dp, me, own, out
        self.send_sem, self.recv_sem = send_sem, recv_sem
        self.half = own.shape[0] // 2
        self.orders = [list(order) + [1] for order in chip_orders(n_dp)]

    def copy(self, color, piece, bit):
        rows = pl.ds(color * self.half, self.half)
        owner = flipped(self.me, piece)
        source = self.own.at[rows] if piece == 0 else self.out.at[owner, rows]
        return pltpu.make_async_remote_copy(
            src_ref=source,
            dst_ref=self.out.at[owner, rows],
            send_sem=self.send_sem.at[color, piece | bit],
            recv_sem=self.recv_sem.at[color, piece | bit],
            device_id={"dp": flipped(self.me, bit)},
            device_id_type=MESH,
        )

    def later(self, color, piece):
        order = self.orders[color]
        last = max((order.index(b) for b in order if piece & b), default=-1)
        return order[last + 1 :]

    def start(self, color, piece):
        for bit in self.later(color, piece):
            self.copy(color, piece, bit).start()

    def arrivals(self, color):
        pieces = [0]
        for bit in self.orders[color]:
            pieces += [p | bit for p in pieces]
        return pieces[1:]

    def last_bit(self, color, piece):
        order = self.orders[color]
        return order[max(order.index(b) for b in order if piece & b)]

    def receive(self, color, piece):
        bit = self.last_bit(color, piece)
        rows = pl.ds(color * self.half, self.half)
        owner = flipped(self.me, piece)
        pltpu.make_async_remote_copy(
            src_ref=self.out.at[owner, rows],
            dst_ref=self.out.at[owner, rows],
            send_sem=self.send_sem.at[color, piece],
            recv_sem=self.recv_sem.at[color, piece],
            device_id={"dp": flipped(self.me, bit)},
            device_id_type=MESH,
        ).wait_recv()

    def drain(self):
        for color in range(2):
            for piece in range(self.n_dp):
                for bit in self.later(color, piece):
                    self.copy(color, piece, bit).wait_send()


class Chain:
    def __init__(self, n_seq, z, own, out, send_sem, recv_sem):
        self.n_seq, self.z, self.own, self.out = n_seq, z, own, out
        self.send_sem, self.recv_sem = send_sem, recv_sem

    def copy(self, way, k):
        shard = self.z - k if way == 0 else self.z + k
        source = self.own if k == 0 else self.out.at[shard]
        return pltpu.make_async_remote_copy(
            src_ref=source,
            dst_ref=self.out.at[shard],
            send_sem=self.send_sem.at[way, k],
            recv_sem=self.recv_sem.at[way, k],
            device_id={"seq": self.z + 1 if way == 0 else self.z - 1},
            device_id_type=MESH,
        )

    def arrived(self, way, k):
        shard = self.z - k if way == 0 else self.z + k
        return pltpu.make_async_remote_copy(
            src_ref=self.out.at[shard],
            dst_ref=self.out.at[shard],
            send_sem=self.send_sem.at[way, k - 1],
            recv_sem=self.recv_sem.at[way, k - 1],
            device_id={"seq": self.z - 1 if way == 0 else self.z + 1},
            device_id_type=MESH,
        )

    def has(self, way, k):
        return self.z >= k if way == 0 else self.z + k <= self.n_seq - 1

    def more(self, way):
        return self.z < self.n_seq - 1 if way == 0 else self.z > 0

    def start(self, k):
        for way in range(2):

            @pl.when(jnp.logical_and(self.has(way, k), self.more(way)))
            def _():
                self.copy(way, k).start()

    def receive(self, k):
        for way in range(2):

            @pl.when(self.has(way, k))
            def _():
                self.arrived(way, k).wait_recv()

            if k < self.n_seq - 1:

                @pl.when(jnp.logical_and(self.has(way, k), self.more(way)))
                def _():
                    self.copy(way, k).start()

    def drain(self):
        for k in range(self.n_seq - 1):
            for way in range(2):

                @pl.when(jnp.logical_and(self.has(way, k), self.more(way)))
                def _():
                    self.copy(way, k).wait_send()


def fetch_kernel(n_dp, n_seq, unit, *refs):
    (x_ref, c_ref, p_ref, up_ref, down_ref) = refs[:5]
    (x_out, c_out, p_out, up_out, down_out) = refs[5:10]
    (up_own, down_own, load_sem, keep_sem, zs, zr, ds, dr) = refs[10:]
    me, z = lax.axis_index("dp"), lax.axis_index("seq")
    ff_own = unit * n_seq
    if up_ref.shape == up_own.shape:
        loads = [pltpu.make_async_copy(up_ref, up_own, load_sem.at[0])]
    else:
        loads = [
            pltpu.make_async_copy(
                up_ref.at[:, pl.ds(pl.multiple_of(d * ff_own + z * unit, 128), unit)],
                up_own.at[:, pl.ds(d * unit, unit)],
                load_sem.at[d],
            )
            for d in range(n_dp)
        ]
    loads.append(
        pltpu.make_async_copy(
            down_ref.at[pl.ds(pl.multiple_of(z * unit, 16), unit)], down_own, load_sem.at[n_dp]
        )
    )
    for load in loads:
        load.start()
    greet(n_dp, n_seq, me, z, True)
    chains = [
        Chain(n_seq, z, own, out, zs.at[i], zr.at[i])
        for i, (own, out) in enumerate(((x_ref, x_out), (c_ref, c_out)))
    ]
    spreads = [
        Spread(n_dp, me, own, out, ds.at[i], dr.at[i])
        for i, (own, out) in enumerate(((p_ref, p_out), (up_own, up_out), (down_own, down_out)))
    ]
    for chain in chains:
        chain.start(0)
    for color in range(2):
        spreads[0].start(color, 0)
    for load in loads[:-1]:
        load.wait()
    for color in range(2):
        spreads[1].start(color, 0)
    loads[-1].wait()
    for color in range(2):
        spreads[2].start(color, 0)
    keeps = [
        pltpu.make_async_copy(own, out.at[at], keep_sem.at[i])
        for i, (own, out, at) in enumerate(
            (
                (x_ref, x_out, z),
                (c_ref, c_out, z),
                (p_ref, p_out, me),
                (up_own, up_out, me),
                (down_own, down_out, me),
            )
        )
    ]
    for keep in keeps:
        keep.start()
    work = []
    for i, spread in enumerate(spreads):
        lists = [spread.arrivals(color) for color in range(2)]
        for at, pair in enumerate(zip(*lists)):
            for color, piece in enumerate(pair):
                when = (piece & ~1).bit_count() + 0.1 * i + 0.5 * (piece & 1)
                work.append((when, at, i, color, piece))
    work.sort()
    rounds = sorted({int(item[0]) for item in work})
    step = 1
    for stage in rounds:
        if step < n_seq:
            for chain in chains:
                chain.receive(step)
            step += 1
        for _, _, i, color, piece in [w for w in work if int(w[0]) == stage]:
            spreads[i].receive(color, piece)
            spreads[i].start(color, piece)
    while step < n_seq:
        for chain in chains:
            chain.receive(step)
        step += 1
    for keep in keeps:
        keep.wait()
    for chain in chains:
        chain.drain()
    for spread in spreads:
        spread.drain()


def fetch(n_dp, n_seq, unit, x, c, params, w_up, w_down):
    rows, width = x.shape
    own = w_up.shape[0]
    if unit % 128:
        w_up = lax.dynamic_index_in_dim(
            w_up.reshape(own, n_dp, n_seq, unit), lax.axis_index("seq"), 2, keepdims=False
        ).reshape(own, n_dp * unit)
    anywhere = pl.BlockSpec(memory_space=pl.ANY)
    inside = pl.BlockSpec(memory_space=pltpu.VMEM)
    return pl.pallas_call(
        functools.partial(fetch_kernel, n_dp, n_seq, unit),
        out_shape=(
            jax.ShapeDtypeStruct((n_seq, rows, width), x.dtype),
            jax.ShapeDtypeStruct((n_seq, rows, width), x.dtype),
            jax.ShapeDtypeStruct((n_dp, *params.shape), params.dtype),
            jax.ShapeDtypeStruct((n_dp, own, n_dp * unit), w_up.dtype),
            jax.ShapeDtypeStruct((n_dp, unit, width), w_down.dtype),
        ),
        in_specs=[inside, inside, inside, anywhere, anywhere],
        out_specs=(anywhere,) * 5,
        scratch_shapes=[
            pltpu.VMEM((own, n_dp * unit), w_up.dtype),
            pltpu.VMEM((unit, width), w_down.dtype),
            pltpu.SemaphoreType.DMA((n_dp + 1,)),
            pltpu.SemaphoreType.DMA((5,)),
            pltpu.SemaphoreType.DMA((2, 2, n_seq)),
            pltpu.SemaphoreType.DMA((2, 2, n_seq)),
            pltpu.SemaphoreType.DMA((3, 2, n_dp)),
            pltpu.SemaphoreType.DMA((3, 2, n_dp)),
        ],
        compiler_params=pltpu.CompilerParams(collective_id=0, has_side_effects=True),
        cost_estimate=pl.CostEstimate(flops=0, bytes_accessed=200_000_000, transcendentals=0),
        name="fetch",
    )(x, c, params, w_up, w_down)


def reduce_kernel(n_dp, n_seq, shapes, *refs):
    count = len(shapes)
    grads, outs = refs[:count], refs[count : 2 * count]
    scratch = refs[2 * count :]
    me, z = lax.axis_index("dp"), lax.axis_index("seq")
    bits = bits_of(n_dp)
    orders = chip_orders(n_dp)
    greet(n_dp, n_seq, me, z, False)

    for i in range(count):
        grad, out = grads[i], outs[i]
        mine, first, load_sem, s0, r0, *stages = scratch[i * (5 + 3 * (bits - 1)) :][
            : 5 + 3 * (bits - 1)
        ]
        half = shapes[i][0] // n_dp // 2

        def rows_of(color, dest):
            return pl.ds(pl.multiple_of((flipped(me, dest) * 2 + color) * half, 8), half)

        def core_copy(color, dest):
            return pltpu.make_async_remote_copy(
                src_ref=grad.at[rows_of(color, dest | 1)],
                dst_ref=first.at[color, dest // 2],
                send_sem=s0.at[color, dest // 2],
                recv_sem=r0.at[color, dest // 2],
                device_id={"dp": flipped(me, 1)},
                device_id_type=MESH,
            )

        def own_load(color, dest):
            return pltpu.make_async_copy(
                grad.at[rows_of(color, dest)], mine.at[color, dest // 2], load_sem.at[color, dest // 2]
            )

        def ranked(color):
            order = orders[color]

            def key(dest):
                return tuple(0 if dest & bit else 1 for bit in order)

            return sorted(range(0, n_dp, 2), key=key)

        for dests in zip(ranked(0), ranked(1)):
            for color, dest in enumerate(dests):
                core_copy(color, dest).start()
                own_load(color, dest).start()

        def stage_copy(color, stage, dest):
            bit = orders[color][stage]
            land, ss, rr = stages[3 * stage : 3 * stage + 3]
            return pltpu.make_async_remote_copy(
                src_ref=mine.at[color, dest // 2],
                dst_ref=land.at[color, slot(color, stage, dest & ~bit)],
                send_sem=ss.at[color, slot(color, stage, dest & ~bit)],
                recv_sem=rr.at[color, slot(color, stage, dest & ~bit)],
                device_id={"dp": flipped(me, bit)},
                device_id_type=MESH,
            )

        def slot(color, stage, dest):
            rest = orders[color][stage + 1 :]
            return sum(1 << k for k, bit in enumerate(rest) if dest & bit)

        def add(color, dest, other, target):
            block = min(16, half)

            def body(step, carry):
                at = pl.ds(pl.multiple_of(step * block, block), block)
                total = mine[color, dest // 2, at, :].astype(jnp.float32) + other[at, :].astype(
                    jnp.float32
                )
                target[at, :] = total.astype(target.dtype)
                return carry

            lax.fori_loop(0, half // block, body, 0)

        for dests in zip(ranked(0), ranked(1)):
            for color, dest in enumerate(dests):
                core_copy(color, dest).wait_recv()
                own_load(color, dest).wait()
                add(color, dest, first.at[color, dest // 2], mine.at[color, dest // 2])
                if dest & orders[color][0]:
                    stage_copy(color, 0, dest).start()
        for stage in range(bits - 1):
            last = stage == bits - 2
            for dests in zip(ranked(0), ranked(1)):
                for color, dest in enumerate(dests):
                    order = orders[color]
                    if any(dest & bit for bit in order[: stage + 1]):
                        continue
                    land = stages[3 * stage]
                    stage_copy(color, stage, dest | order[stage]).wait_recv()
                    place = land.at[color, slot(color, stage, dest)]
                    if last:
                        add(color, dest, place, out.at[pl.ds(color * half, half)])
                    else:
                        add(color, dest, place, mine.at[color, dest // 2])
                        if dest & order[stage + 1]:
                            stage_copy(color, stage + 1, dest).start()
        for color in range(2):
            for dest in range(0, n_dp, 2):
                core_copy(color, dest).wait_send()
                for stage, bit in enumerate(orders[color]):
                    if dest & bit and not any(dest & b for b in orders[color][:stage]):
                        stage_copy(color, stage, dest).wait_send()


def reduce_rows(n_dp, n_seq, ident, *grads):
    bits = bits_of(n_dp)
    anywhere = pl.BlockSpec(memory_space=pl.ANY)
    inside = pl.BlockSpec(memory_space=pltpu.VMEM)
    scratch = []
    for grad in grads:
        rows, cols = grad.shape
        half = rows // n_dp // 2
        kind = grad.dtype
        scratch += [
            pltpu.VMEM((2, n_dp // 2, half, cols), kind),
            pltpu.VMEM((2, n_dp // 2, half, cols), kind),
            pltpu.SemaphoreType.DMA((2, n_dp // 2)),
            pltpu.SemaphoreType.DMA((2, n_dp // 2)),
            pltpu.SemaphoreType.DMA((2, n_dp // 2)),
        ]
        for stage in range(bits - 1):
            left = n_dp // 2 >> (stage + 1)
            scratch += [
                pltpu.VMEM((2, left, half, cols), kind),
                pltpu.SemaphoreType.DMA((2, left)),
                pltpu.SemaphoreType.DMA((2, left)),
            ]
    return pl.pallas_call(
        functools.partial(reduce_kernel, n_dp, n_seq, tuple(g.shape for g in grads)),
        out_shape=tuple(
            jax.ShapeDtypeStruct((g.shape[0] // n_dp, g.shape[1]), g.dtype) for g in grads
        ),
        in_specs=[anywhere] * len(grads),
        out_specs=(inside,) * len(grads),
        scratch_shapes=scratch,
        compiler_params=pltpu.CompilerParams(collective_id=ident, has_side_effects=True),
        cost_estimate=pl.CostEstimate(flops=0, bytes_accessed=100_000_000, transcendentals=0),
        name=f"reduce_{ident}",
    )(*grads)


def dot(a, b, contract):
    return lax.dot_general(a, b, (contract, ((), ())), preferred_element_type=jnp.float32)


def normalize(rows):
    center = rows - jnp.mean(rows, axis=-1, keepdims=True)
    factor = lax.rsqrt(jnp.mean(center * center, axis=-1, keepdims=True) + epsilon)
    return center * factor, factor


def angles(positions):
    half = ROT // 2
    freqs = 10000.0 ** (-2.0 * jnp.arange(half).astype(positions.dtype) / ROT)
    theta = positions[:, None] * freqs[None, :]
    return (jnp.cos(theta), jnp.sin(theta))


def rotate(tensor, cosine, sine, direction):
    half = ROT // 2
    first_half = tensor[..., :half]
    second_half = tensor[..., half:ROT]
    return jnp.concatenate(
        [
            first_half * cosine - direction * second_half * sine,
            second_half * cosine + direction * first_half * sine,
            tensor[..., ROT:],
        ],
        axis=-1,
    )


def gather_dp(rows):
    return lax.all_gather(rows, "dp", axis=0, tiled=True)


def gather_seq(shard):
    return lax.all_gather(shard, "seq", axis=0, tiled=False)


def exchange_sum(partial, n_seq):
    slabs = partial.astype(jnp.bfloat16).reshape(n_seq, partial.shape[0] // n_seq, partial.shape[1])
    got = lax.all_to_all(slabs, "seq", split_axis=0, concat_axis=0, tiled=True)
    return jnp.sum(got.astype(jnp.float32), axis=0)


def make_local(n_dp, n_seq):
    def local(
        layer_input,
        cotangent,
        ln1_gain,
        ln1_bias,
        w_qkv,
        b_qkv,
        w_out,
        b_out,
        ln2_gain,
        ln2_bias,
        w_up,
        b_up,
        w_down,
        b_down,
    ):
        f32, bf16 = jnp.float32, jnp.bfloat16
        _, tok_local, width = layer_input.shape
        length = tok_local * n_seq
        own = width // n_dp
        ff = w_up.shape[1]
        ff_own = ff // n_dp
        unit = ff_own // n_seq
        heads = H // n_seq
        z = lax.axis_index("seq")

        qkv_own = lax.dynamic_slice_in_dim(
            w_qkv.reshape(own, 3, H, HD), z * heads, heads, 2
        ).reshape(own, 3 * heads * HD)
        triple_w = gather_dp(qkv_own)
        owners = n_dp // n_seq
        piece = own // n_dp
        spread = lax.all_to_all(
            w_out.reshape(n_dp, piece, width), "dp", split_axis=0, concat_axis=0, tiled=True
        )
        out_own = lax.dynamic_slice_in_dim(spread, z * owners, owners, 0)
        out_w = (
            lax.all_gather(out_own, "dp", axis=0, tiled=False)
            .transpose(1, 0, 2, 3)
            .reshape(owners * own, width)
        )

        packed = jnp.concatenate(
            [ln1_gain, ln1_bias, ln2_gain, ln2_bias, b_out, b_down, b_qkv, b_up]
        )
        packed = jnp.pad(packed, (0, -packed.shape[0] % 2048)).reshape(-1, 128)
        tokens, incoming, gathered, up_w, down_w = fetch(
            n_dp,
            n_seq,
            unit,
            layer_input.reshape(tok_local, width),
            cotangent.reshape(tok_local, width),
            packed,
            w_up,
            w_down,
        )
        tokens, incoming = tokens.reshape(length, width), incoming.reshape(length, width)
        gathered = gathered.reshape(n_dp, -1)
        up_w = up_w.reshape(width, n_dp * unit)
        down_w = down_w.reshape(n_dp * unit, width)
        gain_one, shift_one, gain_two, shift_two, out_b, down_b = (
            gathered[:, k * own : (k + 1) * own].reshape(width) for k in range(6)
        )
        base = 6 * own
        triple_b = lax.dynamic_slice_in_dim(
            gathered[:, base : base + 3 * own].reshape(3, H, HD), z * heads, heads, 1
        ).reshape(3 * heads * HD)
        up_b = lax.dynamic_index_in_dim(
            gathered[:, base + 3 * own : base + 3 * own + ff_own].reshape(n_dp, n_seq, unit), z, 1, keepdims=False
        ).reshape(n_dp * unit)

        normed, _ = normalize(tokens.astype(f32))
        mlp_in = (normed * gain_two + shift_two).astype(bf16)
        attn_in = (normed * gain_one + shift_one).astype(bf16)

        inner = dot(mlp_in, up_w, ((1,), (0,))) + up_b
        cumulative = 0.5 * (1.0 + lax.erf(inner * 0.7071067811865476))
        hidden = (inner * cumulative).astype(bf16)
        slope = cumulative + inner * jnp.exp(-0.5 * inner * inner) * 0.3989422804014327
        down_grad = dot(hidden, incoming, ((0,), (0,))).astype(bf16)
        inner_grad = dot(incoming, down_w, ((1,), (1,))) * slope
        inner_grad_b = inner_grad.astype(bf16)
        up_grad = dot(mlp_in, inner_grad_b, ((0,), (0,))).astype(bf16)
        mlp_out = dot(hidden, down_w, ((1,), (0,)))
        mlp_in_grad = dot(inner_grad_b, up_w, ((1,), (1,)))
        b_up_grad = jnp.sum(inner_grad, axis=0)
        ln2_gain_grad = jnp.sum(mlp_in_grad * normed, axis=0)
        ln2_bias_grad = jnp.sum(mlp_in_grad, axis=0)

        cosine, sine = angles(jnp.arange(length, dtype=jnp.int32).astype(f32))
        cosine, sine = cosine[:, None, :], sine[:, None, :]
        triple = (dot(attn_in, triple_w, ((1,), (0,))) + triple_b).reshape(length, 3, heads, HD)
        queries = rotate(triple[:, 0], cosine, sine, 1.0).astype(bf16)
        key_rows = rotate(triple[:, 1], cosine, sine, 1.0).astype(bf16)
        values = triple[:, 2].astype(bf16)
        scores = jnp.einsum("qhd,khd->hqk", queries, key_rows, preferred_element_type=f32) * HD ** (
            -0.5
        )
        order = jnp.arange(length, dtype=jnp.int32)
        scores = jnp.where((order[None, :] <= order[:, None])[None], scores, masked_fill)
        top = jnp.max(scores, axis=-1, keepdims=True)
        logsum = top + jnp.log(jnp.sum(jnp.exp(scores - top), axis=-1, keepdims=True))
        probs_f = jnp.exp(scores - logsum)
        probs = probs_f.astype(bf16)
        context = jnp.einsum("hqk,khd->qhd", probs, values, preferred_element_type=f32).astype(bf16)
        merged = context.reshape(length, heads * HD)
        attended = dot(merged, out_w, ((1,), (0,)))
        out_grad = dot(merged, incoming, ((0,), (0,))).astype(bf16)
        context_grad = dot(incoming, out_w, ((1,), (1,))).astype(bf16).reshape(length, heads, HD)
        delta = jnp.sum(context_grad.astype(f32) * context.astype(f32), axis=-1)
        value_grad = jnp.einsum(
            "hqk,qhd->khd", probs, context_grad, preferred_element_type=f32
        ).astype(bf16)
        prob_grad = jnp.einsum("qhd,khd->hqk", context_grad, values, preferred_element_type=f32)
        score_grad = (probs_f * (prob_grad - delta.T[:, :, None]) * HD ** (-0.5)).astype(bf16)
        query_grad = jnp.einsum(
            "hqk,khd->qhd", score_grad, key_rows, preferred_element_type=f32
        ).astype(bf16)
        key_grad = jnp.einsum(
            "hqk,qhd->khd", score_grad, queries, preferred_element_type=f32
        ).astype(bf16)
        triple_grad = jnp.stack(
            [
                rotate(query_grad.astype(f32), cosine, sine, -1.0),
                rotate(key_grad.astype(f32), cosine, sine, -1.0),
                value_grad.astype(f32),
            ],
            axis=1,
        ).reshape(length, 3 * heads * HD)
        triple_grad_b = triple_grad.astype(bf16)
        b_qkv_grad = jnp.sum(triple_grad, axis=0)
        qkv_grad = dot(attn_in, triple_grad_b, ((0,), (0,))).astype(bf16)
        attn_in_grad = dot(triple_grad_b, triple_w, ((1,), (1,)))
        ln1_gain_grad = jnp.sum(attn_in_grad * normed, axis=0)
        ln1_bias_grad = jnp.sum(attn_in_grad, axis=0)

        rows = layer_input.reshape(tok_local, width).astype(f32)
        grad_rows = cotangent.reshape(tok_local, width).astype(f32)
        output = rows + (out_b + down_b) + exchange_sum(attended + mlp_out, n_seq)
        scaled = exchange_sum(attn_in_grad * gain_one + mlp_in_grad * gain_two, n_seq)
        normed_own, factor_own = normalize(rows)
        input_grad = grad_rows + factor_own * (
            scaled
            - jnp.mean(scaled, axis=-1, keepdims=True)
            - normed_own * jnp.mean(scaled * normed_own, axis=-1, keepdims=True)
        )

        here = jnp.arange(n_seq) == z
        b_up_wide = jnp.where(
            here[None, :, None], b_up_grad.reshape(n_dp, 1, unit), 0.0
        ).reshape(n_dp, ff_own)
        b_qkv_wide = jnp.where(
            here[None, :, None], b_qkv_grad.reshape(3, 1, heads * HD), 0.0
        ).reshape(n_dp, 3 * own)
        b_down_grad = jnp.sum(grad_rows, axis=0)
        small = jnp.concatenate(
            [
                ln1_gain_grad.reshape(n_dp, own),
                ln1_bias_grad.reshape(n_dp, own),
                ln2_gain_grad.reshape(n_dp, own),
                ln2_bias_grad.reshape(n_dp, own),
                b_down_grad.reshape(n_dp, own),
                b_qkv_wide,
                b_up_wide,
            ],
            axis=1,
        )
        small_len = small.shape[1]
        small = jnp.pad(small, ((0, 0), (0, -small_len % 4096))).reshape(-1, 256)

        (down_sum,) = reduce_rows(n_dp, n_seq, 1, down_grad)
        down_full = gather_seq(down_sum).reshape(ff_own, width).astype(f32)
        (up_sum,) = reduce_rows(n_dp, n_seq, 2, up_grad)
        up_full = (
            gather_seq(up_sum)
            .reshape(n_seq, own, n_dp, unit)
            .transpose(1, 2, 0, 3)
            .reshape(own, ff)
        ).astype(f32)
        out_sum, small_sum = reduce_rows(
            n_dp,
            n_seq,
            3,
            out_grad.reshape(owners, n_dp, piece, width)
            .transpose(1, 0, 2, 3)
            .reshape(n_dp * owners * piece, width),
            small,
        )
        few = owners * piece
        small_sum = small_sum.reshape(-1, width).astype(bf16)
        extra = small_sum.shape[0]
        tail = jnp.pad(small_sum, ((0, -extra % 16), (0, 0)))
        out_part = gather_seq(jnp.concatenate([out_sum, tail], axis=0))
        out_full = (
            lax.all_to_all(
                out_part[:, :few].reshape(n_dp, piece, width),
                "dp",
                split_axis=0,
                concat_axis=0,
                tiled=True,
            )
            .reshape(own, width)
            .astype(f32)
        )
        mine = jnp.sum(out_part[:, few : few + extra].astype(f32), axis=0).reshape(-1)
        g1, s1, g2, s2, bd = (mine[k * own : (k + 1) * own] for k in range(5))
        bq = mine[5 * own : 8 * own]
        bu = mine[8 * own : small_len]
        (qkv_sum,) = reduce_rows(n_dp, n_seq, 4, qkv_grad)
        qkv_full = (
            gather_seq(qkv_sum)
            .reshape(n_seq, own, 3, heads * HD)
            .transpose(1, 2, 0, 3)
            .reshape(own, 3 * width)
            .astype(f32)
        )

        return (
            output.reshape(layer_input.shape),
            input_grad.reshape(layer_input.shape),
            g1,
            s1,
            qkv_full,
            bq,
            out_full,
            bd,
            g2,
            s2,
            up_full,
            bu,
            down_full,
            bd,
        )

    return local


def solution(mesh):
    vector, matrix, tokens = P("dp"), P("dp", None), P("dp", "seq", None)
    in_specs = (
        tokens,
        tokens,
        vector,
        vector,
        matrix,
        vector,
        matrix,
        vector,
        vector,
        vector,
        matrix,
        vector,
        matrix,
        vector,
    )
    out_specs = (
        tokens,
        tokens,
        vector,
        vector,
        matrix,
        vector,
        matrix,
        vector,
        vector,
        vector,
        matrix,
        vector,
        matrix,
        vector,
    )
    local = make_local(mesh.shape["dp"], mesh.shape["seq"])
    return jax.shard_map(
        local, mesh=mesh, in_specs=in_specs, out_specs=out_specs, check_vma=False
    )
```

```python
import functools

import jax
import jax.numpy as jnp
from jax import lax
from jax.experimental import pallas as pl
from jax.experimental.pallas import tpu as pltpu
from jax.sharding import PartitionSpec as P


H = 8
HD = 256
ROT = 64

epsilon = 1e-05
masked_fill = -1e30

MESH = pl.DeviceIdType.MESH
ANYWHERE = pl.BlockSpec(memory_space=pl.ANY)
INSIDE = pl.BlockSpec(memory_space=pltpu.VMEM)


def dot(a, b, contract):
    return lax.dot_general(a, b, (contract, ((), ())), preferred_element_type=jnp.float32)


def tile(index, size):
    start = index * size
    return pl.ds(start if isinstance(start, int) else pl.multiple_of(start, size), size)


def guarded(condition, body):
    if condition is None:
        body()
    else:
        pl.when(condition)(body)


def bits_of(n):
    return n.bit_length() - 1


def flipped(me, mask):
    for k in range(mask.bit_length()):
        if mask >> k & 1:
            me = me + (1 << k) * (1 - 2 * ((me // (1 << k)) % 2))
    return me


def chip_orders(n):
    chips = [1 << k for k in range(1, bits_of(n))]
    return chips, chips[1:] + chips[:1]


def greet(n_dp, n_seq, me, z, everyone=False):
    barrier = pltpu.get_barrier_semaphore()
    masks = range(1, n_dp) if everyone else [1 << k for k in range(bits_of(n_dp))]
    for mask in masks:
        pl.semaphore_signal(
            barrier, inc=1, device_id={"dp": flipped(me, mask)}, device_id_type=MESH
        )
    peers = len(masks)
    if n_seq > 1:

        @pl.when(z > 0)
        def _():
            pl.semaphore_signal(barrier, inc=1, device_id={"seq": z - 1}, device_id_type=MESH)

        @pl.when(z < n_seq - 1)
        def _():
            pl.semaphore_signal(barrier, inc=1, device_id={"seq": z + 1}, device_id_type=MESH)

        peers = peers + (z + n_seq - 1) // n_seq + (2 * n_seq - 2 - z) // n_seq
    pl.semaphore_wait(barrier, peers)


def in_turn(*lists):
    lists = [list(steps) for steps in lists]
    while any(lists):
        for steps in lists:
            if steps:
                steps.pop(0)()


class Spread:
    def __init__(self, n_dp, me, own, out, sems, held_by=None, slot=None):
        self.n_dp, self.me, self.own, self.out = n_dp, me, own, out
        self.send_sem, self.recv_sem = sems
        self.half = own.shape[0] // 2
        self.orders = [list(order) + [1] for order in chip_orders(n_dp)]
        self.held_by = held_by or (lambda owner: None)
        self.slot = slot or (lambda owner: owner)

    @staticmethod
    def sems(n_dp):
        return [pltpu.SemaphoreType.DMA((2, n_dp)), pltpu.SemaphoreType.DMA((2, n_dp))]

    def place(self, color, piece):
        owner = flipped(self.me, piece)
        return self.out.at[self.slot(owner), pl.ds(color * self.half, self.half)]

    def copy(self, color, piece, bit, arrived=False):
        if arrived or piece:
            source = self.place(color, piece)
        else:
            source = self.own.at[pl.ds(color * self.half, self.half)]
        key = piece if arrived else piece | bit
        return pltpu.make_async_remote_copy(
            src_ref=source,
            dst_ref=self.place(color, piece),
            send_sem=self.send_sem.at[color, key],
            recv_sem=self.recv_sem.at[color, key],
            device_id={"dp": flipped(self.me, bit)},
            device_id_type=MESH,
        )

    def later(self, color, piece):
        order = self.orders[color]
        last = max((order.index(b) for b in order if piece & b), default=-1)
        return order[last + 1 :]

    def start(self, color, piece=0):
        def body():
            for bit in self.later(color, piece):
                self.copy(color, piece, bit).start()

        guarded(self.held_by(flipped(self.me, piece)), body)

    def begin(self):
        for color in range(2):
            self.start(color)

    def receive(self, color, piece):
        order = self.orders[color]
        bit = order[max(order.index(b) for b in order if piece & b)]

        def body():
            self.copy(color, piece, bit, arrived=True).wait_recv()

        guarded(self.held_by(flipped(self.me, piece)), body)

    def arrivals(self):
        lists = []
        for order in self.orders:
            pieces = [0]
            for bit in order:
                pieces += [p | bit for p in pieces]
            lists.append(pieces[1:])
        return lists

    def steps(self):
        for pair in zip(*self.arrivals()):
            for color, piece in enumerate(pair):

                def step(color=color, piece=piece):
                    self.receive(color, piece)
                    self.start(color, piece)

                yield step

    def finish(self):
        for color in range(2):
            for piece in range(self.n_dp):

                def body():
                    for bit in self.later(color, piece):
                        self.copy(color, piece, bit).wait_send()

                guarded(self.held_by(flipped(self.me, piece)), body)


class Chain:
    def __init__(self, n_seq, z, own, out, sems):
        self.n_seq, self.z, self.own, self.out = n_seq, z, own, out
        self.send_sem, self.recv_sem = sems

    @staticmethod
    def sems(n_seq):
        return [pltpu.SemaphoreType.DMA((2, n_seq)), pltpu.SemaphoreType.DMA((2, n_seq))]

    def copy(self, way, k, arrived=False):
        shard = self.z - k if way == 0 else self.z + k
        source = self.own if k == 0 else self.out.at[shard]
        key = k - 1 if arrived else k
        return pltpu.make_async_remote_copy(
            src_ref=source,
            dst_ref=self.out.at[shard],
            send_sem=self.send_sem.at[way, key],
            recv_sem=self.recv_sem.at[way, key],
            device_id={"seq": self.z + 1 if (way == 0) != arrived else self.z - 1},
            device_id_type=MESH,
        )

    def has(self, way, k):
        return self.z >= k if way == 0 else self.z + k <= self.n_seq - 1

    def more(self, way):
        return self.z < self.n_seq - 1 if way == 0 else self.z > 0

    def sends(self, way, k):
        return jnp.logical_and(self.has(way, k), self.more(way))

    def begin(self):
        for way in range(2):
            pl.when(self.sends(way, 0))(lambda: self.copy(way, 0).start())

    def steps(self):
        for k in range(1, self.n_seq):
            for way in range(2):

                def step(k=k, way=way):
                    pl.when(self.has(way, k))(lambda: self.copy(way, k, True).wait_recv())
                    if k < self.n_seq - 1:
                        pl.when(self.sends(way, k))(lambda: self.copy(way, k).start())

                yield step

    def finish(self):
        for k in range(self.n_seq - 1):
            for way in range(2):
                pl.when(self.sends(way, k))(lambda: self.copy(way, k).wait_send())


class Cast:
    def __init__(self, n_seq, z, origin, own, out, sems, pieces):
        self.n_seq, self.z, self.origin, self.own, self.out = n_seq, z, origin, own, out
        self.send_sem, self.recv_sem = sems
        self.pieces, self.rows = pieces, own.shape[0] // pieces

    @staticmethod
    def sems(pieces):
        return [pltpu.SemaphoreType.DMA((2, pieces)), pltpu.SemaphoreType.DMA((2, pieces))]

    def copy(self, way, piece, source, arrived=False):
        at = pl.ds(piece * self.rows, self.rows)
        return pltpu.make_async_remote_copy(
            src_ref=source.at[at],
            dst_ref=self.out.at[at],
            send_sem=self.send_sem.at[way, piece],
            recv_sem=self.recv_sem.at[way, piece],
            device_id={"seq": self.z + 1 if (way == 0) != arrived else self.z - 1},
            device_id_type=MESH,
        )

    def more(self, way):
        return self.z < self.n_seq - 1 if way == 0 else self.z > 0

    def sends(self, way, first):
        if first:
            here = self.z == self.origin
        else:
            here = self.z > self.origin if way == 0 else self.z < self.origin
        return jnp.logical_and(here, self.more(way))

    def begin(self):
        for piece in range(self.pieces):
            for way in range(2):
                pl.when(self.sends(way, True))(lambda: self.copy(way, piece, self.own).start())

    def steps(self):
        for piece in range(self.pieces):
            for way in range(2):

                def step(piece=piece, way=way):
                    got = self.z > self.origin if way == 0 else self.z < self.origin
                    pl.when(got)(lambda: self.copy(way, piece, self.out, True).wait_recv())
                    pl.when(self.sends(way, False))(
                        lambda: self.copy(way, piece, self.out).start()
                    )

                yield step

    def finish(self):
        for piece in range(self.pieces):
            for way in range(2):
                for first in (True, False):
                    pl.when(self.sends(way, first))(
                        lambda: self.copy(way, piece, self.out).wait_send()
                    )


class Direct:
    def __init__(self, n_dp, me, own, out, sems):
        self.n_dp, self.me, self.own, self.out = n_dp, me, own, out
        self.send_sem, self.recv_sem = sems

    @staticmethod
    def sems(n_dp):
        return [pltpu.SemaphoreType.DMA((n_dp,)), pltpu.SemaphoreType.DMA((n_dp,))]

    def copy(self, mask, owner):
        return pltpu.make_async_remote_copy(
            src_ref=self.own,
            dst_ref=self.out.at[owner],
            send_sem=self.send_sem.at[mask],
            recv_sem=self.recv_sem.at[mask],
            device_id={"dp": flipped(self.me, mask)},
            device_id_type=MESH,
        )

    def begin(self):
        for mask in range(1, self.n_dp):
            self.copy(mask, self.me).start()

    def receive(self):
        for mask in range(1, self.n_dp):
            self.copy(mask, flipped(self.me, mask)).wait_recv()

    def finish(self):
        for mask in range(1, self.n_dp):
            self.copy(mask, self.me).wait_send()


class Scatter:
    def __init__(self, n_dp, owners, me, z, rows, out, sems):
        self.n_dp, self.owners, self.me, self.z, self.rows, self.out = n_dp, owners, me, z, rows, out
        self.send_sem, self.recv_sem = sems
        self.piece = rows.shape[0] // n_dp

    @staticmethod
    def sems(n_dp, owners):
        return [pltpu.SemaphoreType.DMA((n_dp,)), pltpu.SemaphoreType.DMA((owners,))]

    def source(self, dest):
        return self.rows.at[pl.ds(pl.multiple_of(dest * self.piece, self.piece), self.piece)]

    def copy(self, mask, slot):
        dest = flipped(self.me, mask)
        return pltpu.make_async_remote_copy(
            src_ref=self.source(dest),
            dst_ref=self.out.at[slot],
            send_sem=self.send_sem.at[mask],
            recv_sem=self.recv_sem.at[slot],
            device_id={"dp": dest},
            device_id_type=MESH,
        )

    def keep(self):
        return pltpu.make_async_copy(
            self.source(self.me), self.out.at[self.me % self.owners], self.send_sem.at[0]
        )

    def when(self, body):
        pl.when(self.me // self.owners == self.z)(body)

    def begin(self):
        def body():
            for mask in range(1, self.n_dp):
                self.copy(mask, self.me % self.owners).start()
            self.keep().start()

        self.when(body)

    def finish(self):
        for slot in range(self.owners):
            pl.when(self.z * self.owners + slot != self.me)(
                lambda: self.copy(1, slot).wait_recv()
            )

        def body():
            for mask in range(1, self.n_dp):
                self.copy(mask, self.me % self.owners).wait_send()
            self.keep().wait()

        self.when(body)


class Reduce:
    def __init__(self, n_dp, me, grad, out, scratch, rows_at=None, held_by=None, make=None):
        self.n_dp, self.me, self.grad, self.out = n_dp, me, grad, out
        self.mine, self.first, self.load_sem, self.s0, self.r0, *self.stages = scratch
        self.half = out.shape[0] // 2
        self.orders = chip_orders(n_dp)
        self.rows_at = rows_at or (lambda dest: 2 * dest)
        self.held_by = held_by or (lambda dest: None)
        self.make = make
        self.dests = sorted(range(0, n_dp, 2), key=lambda d: -d.bit_count())

    @staticmethod
    def scratch(n_dp, half, cols, kind, made=False):
        pairs = n_dp // 2
        result = [
            pltpu.VMEM((2 if made else 1, 2, pairs, half, cols), kind),
            pltpu.VMEM((2, pairs, half, cols), kind),
            pltpu.SemaphoreType.DMA((2, pairs)),
            pltpu.SemaphoreType.DMA((2, pairs)),
            pltpu.SemaphoreType.DMA((2, pairs)),
        ]
        for stage in range(bits_of(n_dp) - 1):
            left = pairs >> (stage + 1)
            result += [
                pltpu.VMEM((2, left, half, cols), kind),
                pltpu.SemaphoreType.DMA((2, left)),
                pltpu.SemaphoreType.DMA((2, left)),
            ]
        return result

    def kept(self, color, dest):
        core = self.me % 2 if self.make else 0
        return self.mine.at[core, color, dest // 2]

    def when(self, dest, body):
        guarded(self.held_by(flipped(self.me, dest)), body)

    def source(self, color, dest):
        start = (self.rows_at(flipped(self.me, dest)) + color) * self.half
        return self.grad.at[pl.ds(pl.multiple_of(start, self.half), self.half)]

    def core_copy(self, color, dest):
        if self.make:
            source = self.mine.at[1 - self.me % 2, color, dest // 2]
        else:
            source = self.source(color, dest | 1)
        return pltpu.make_async_remote_copy(
            src_ref=source,
            dst_ref=self.first.at[color, dest // 2],
            send_sem=self.s0.at[color, dest // 2],
            recv_sem=self.r0.at[color, dest // 2],
            device_id={"dp": flipped(self.me, 1)},
            device_id_type=MESH,
        )

    def own_load(self, color, dest):
        return pltpu.make_async_copy(
            self.source(color, dest), self.kept(color, dest), self.load_sem.at[color, dest // 2]
        )

    def slot(self, color, stage, dest):
        rest = self.orders[color][stage + 1 :]
        return sum(1 << k for k, bit in enumerate(rest) if dest & bit)

    def stage_copy(self, color, stage, dest):
        bit = self.orders[color][stage]
        land, ss, rr = self.stages[3 * stage : 3 * stage + 3]
        at = self.slot(color, stage, dest & ~bit)
        return pltpu.make_async_remote_copy(
            src_ref=self.kept(color, dest),
            dst_ref=land.at[color, at],
            send_sem=ss.at[color, at],
            recv_sem=rr.at[color, at],
            device_id={"dp": flipped(self.me, bit)},
            device_id_type=MESH,
        )

    def add(self, color, dest, other, target):
        block = min(16, self.half)
        kept = self.kept(color, dest)

        def body(step, carry):
            at = pl.ds(pl.multiple_of(step * block, block), block)
            total = kept[at, :].astype(jnp.float32) + other[at, :].astype(jnp.float32)
            target[at, :] = total.astype(target.dtype)
            return carry

        lax.fori_loop(0, self.half // block, body, 0)

    def begin(self):
        if not self.make:
            for dest in self.dests:
                self.give(dest)

    def give(self, dest):
        if self.make:
            half = self.half

            def store(core, columns, values):
                for color in range(2):
                    self.mine[core, color, dest // 2, :, columns] = values[
                        color * half : (color + 1) * half
                    ].astype(self.mine.dtype)

            self.make(flipped(self.me, dest) // 2, store)

        def body():
            for color in range(2):
                self.core_copy(color, dest).start()
                if not self.make:
                    self.own_load(color, dest).start()

        self.when(dest, body)

    def meet(self, dest):
        def body():
            for color in range(2):
                self.core_copy(color, dest).wait_recv()
                if not self.make:
                    self.own_load(color, dest).wait()
                self.add(
                    color, dest, self.first.at[color, dest // 2], self.kept(color, dest)
                )
                if dest & self.orders[color][0]:
                    self.stage_copy(color, 0, dest).start()

        self.when(dest, body)

    def merge(self, stage, color, dest):
        order = self.orders[color]

        def body():
            self.stage_copy(color, stage, dest | order[stage]).wait_recv()
            place = self.stages[3 * stage].at[color, self.slot(color, stage, dest)]
            if stage == len(order) - 1:
                self.add(color, dest, place, self.out.at[pl.ds(color * self.half, self.half)])
            else:
                self.add(color, dest, place, self.kept(color, dest))
                if dest & order[stage + 1]:
                    self.stage_copy(color, stage + 1, dest).start()

        self.when(dest, body)

    def steps(self):
        gives = [functools.partial(self.give, dest) for dest in self.dests] if self.make else []
        meets = [functools.partial(self.meet, dest) for dest in self.dests]
        while gives or meets:
            if gives:
                yield gives.pop(0)
            if len(gives) < len(meets) - 1 or not gives:
                yield meets.pop(0)
        for stage in range(len(self.orders[0])):
            for dest in self.dests:
                for color in range(2):
                    if not any(dest & bit for bit in self.orders[color][: stage + 1]):
                        yield functools.partial(self.merge, stage, color, dest)

    def finish(self):
        for dest in self.dests:

            def body():
                for color in range(2):
                    self.core_copy(color, dest).wait_send()

            self.when(dest, body)
            for color in range(2):
                for stage, bit in enumerate(self.orders[color]):
                    if dest & bit and not any(dest & b for b in self.orders[color][:stage]):
                        self.when(
                            dest, lambda: self.stage_copy(color, stage, dest).wait_send()
                        )


class Settle:
    def __init__(self, n_seq, z, partial, out, scratch):
        self.n_seq, self.z, self.partial, self.out = n_seq, z, partial, out
        self.land, self.stage, self.send_sem, self.recv_sem = scratch

    @staticmethod
    def scratch(n_seq, rows, width, kind):
        return [
            pltpu.VMEM((2, n_seq - 1, rows, width), kind),
            pltpu.VMEM((2, n_seq - 2, rows, width), kind),
            pltpu.SemaphoreType.DMA((2, n_seq - 1)),
            pltpu.SemaphoreType.DMA((2, n_seq - 1)),
        ]

    def slab(self, way, k):
        return self.z + k if way == 0 else self.z - k

    def copy(self, way, k, source):
        return pltpu.make_async_remote_copy(
            src_ref=source,
            dst_ref=self.land.at[way, k - 1],
            send_sem=self.send_sem.at[way, k - 1],
            recv_sem=self.recv_sem.at[way, k - 1],
            device_id={"seq": self.z + 1 if way == 0 else self.z - 1},
            device_id_type=MESH,
        )

    def first(self, way):
        return self.z == 0 if way == 0 else self.z == self.n_seq - 1

    def reaches(self, way, k):
        return self.z + k <= self.n_seq - 1 if way == 0 else self.z >= k

    def each(self, body):
        block = 16

        def step(i, carry):
            body(pl.ds(pl.multiple_of(i * block, block), block))
            return carry

        lax.fori_loop(0, self.out.shape[0] // block, step, 0)

    def begin(self):
        for k in range(self.n_seq - 1, 0, -1):
            for way in range(2):
                pl.when(jnp.logical_and(self.first(way), self.reaches(way, k)))(
                    lambda: self.copy(way, k, self.partial.at[self.slab(way, k)]).start()
                )

    def pass_on(self, way, k):
        def body():
            self.copy(way, k + 1, self.land.at[way, k]).wait_recv()

            def add(at):
                total = self.partial[self.slab(way, k), at, :].astype(jnp.float32) + self.land[
                    way, k, at, :
                ].astype(jnp.float32)
                self.stage[way, k - 1, at, :] = total.astype(self.stage.dtype)

            self.each(add)
            self.copy(way, k, self.stage.at[way, k - 1]).start()

        pl.when(jnp.logical_and(jnp.logical_not(self.first(way)), self.reaches(way, k)))(body)

    def keep(self):
        def add(at):
            self.out[at, :] = self.partial[self.z, at, :].astype(jnp.float32)

        self.each(add)

    def close(self, way):
        def body():
            self.copy(way, 1, self.land.at[way, 0]).wait_recv()

            def add(at):
                self.out[at, :] += self.land[way, 0, at, :].astype(jnp.float32)

            self.each(add)

        pl.when(jnp.logical_not(self.first(way)))(body)

    def steps(self):
        for k in range(self.n_seq - 2, 0, -1):
            for way in range(2):
                yield functools.partial(self.pass_on, way, k)
        yield self.keep
        for way in range(2):
            yield functools.partial(self.close, way)

    def finish(self):
        for k in range(self.n_seq - 1, 0, -1):
            for way in range(2):
                pl.when(self.reaches(way, k))(
                    lambda: self.copy(way, k, self.land.at[way, k - 1]).wait_send()
                )


def take(refs, *counts):
    groups, at = [], 0
    for count in counts:
        groups.append(refs[at : at + count])
        at += count
    return groups


def remote_call(ident, body, outs, out_specs, in_specs, scratch, args):
    return pl.pallas_call(
        body,
        out_shape=tuple(outs),
        in_specs=in_specs,
        out_specs=tuple(out_specs),
        scratch_shapes=scratch,
        compiler_params=pltpu.CompilerParams(collective_id=ident, has_side_effects=True),
        cost_estimate=pl.CostEstimate(flops=0, bytes_accessed=100_000_000, transcendentals=0),
    )(*args)


def load_all(pairs, sems):
    loads = [
        pltpu.make_async_copy(source, target, sems.at[i])
        for i, (source, target) in enumerate(pairs)
    ]
    for load in loads:
        load.start()
    return loads


def woven(steps, compute, count, first=0):
    steps = list(steps)

    def body(j, carry):
        compute(j)
        done = 0
        for i in range(first, count):
            upto = len(steps) * (i + 1 - first) // (count - first)
            if upto > done:
                pl.when(j == i)(lambda: [step() for step in steps[done:upto]] and None)
            done = upto
        return carry

    lax.fori_loop(0, count, body, 0)


def fetch(n_dp, n_seq, unit, x, c, params, w_up, w_down, w_out):
    f32, bf16 = jnp.float32, jnp.bfloat16
    rows, width = x.shape
    own = w_up.shape[0]
    units = n_dp * unit
    length = n_seq * rows
    owners = n_dp // n_seq
    lines = own // 128
    whole = unit % 128 == 0 and own % 128 == 0
    if not whole:
        w_up = lax.dynamic_index_in_dim(
            w_up.reshape(own, n_dp, n_seq, unit), lax.axis_index("seq"), 2, keepdims=False
        ).reshape(own, units)
    extra = 4 if whole else 0

    def body(*refs):
        ins, outs, made, own_scratch, inner_scratch, sems = take(
            refs, 6, 6, extra, 4, 3 if whole else 0, 12
        )
        x_ref, c_ref, p_ref, up_ref, down_ref, out_ref = ins
        x_all, c_all, p_all, up_all, down_all, out_piece = outs
        up_own, down_own, load_sem, keep_sem = own_scratch
        me, z = lax.axis_index("dp"), lax.axis_index("seq")
        if whole:
            pairs = [
                (
                    up_ref.at[:, pl.ds(pl.multiple_of((d * n_seq + z) * unit, 128), unit)],
                    up_own.at[:, pl.ds(d * unit, unit)],
                )
                for d in range(n_dp)
            ]
        else:
            pairs = [(up_ref, up_own)]
        loads = load_all([*pairs, (down_ref.at[tile(z, unit)], down_own)], load_sem)
        greet(n_dp, n_seq, me, z, everyone=True)
        chains = [
            Chain(n_seq, z, source, out, sems[2 * i : 2 * i + 2])
            for i, (source, out) in enumerate(((x_ref, x_all), (c_ref, c_all)))
        ]
        up, down = (
            Spread(n_dp, me, source, out, sems[4 + 2 * i : 6 + 2 * i])
            for i, (source, out) in enumerate(((up_own, up_all), (down_own, down_all)))
        )
        direct = Direct(n_dp, me, p_ref, p_all, sems[8:10])
        scatter = Scatter(n_dp, owners, me, z, out_ref, out_piece, sems[10:12])
        direct.begin()
        chains[0].begin()
        chains[1].begin()
        for load in loads[:-1]:
            load.wait()
        up.begin()
        x_keep, c_keep, p_keep, up_keep, down_keep = (
            pltpu.make_async_copy(source, out.at[at], keep_sem.at[i])
            for i, (source, out, at) in enumerate(
                (
                    (x_ref, x_all, z),
                    (c_ref, c_all, z),
                    (p_ref, p_all, me),
                    (up_own, up_all, me),
                    (down_own, down_all, me),
                )
            )
        )
        keeps = (x_keep, c_keep, p_keep, up_keep, down_keep)
        for keep in keeps[:4]:
            keep.start()

        if whole:
            mlp_in, attn_in, hidden, slope = made
            up_v, vectors, place_sem = inner_scratch

            def placed(color, piece):
                owner = flipped(me, piece)
                at = pl.ds(
                    pl.multiple_of(owner * own + color * (own // 2), own // 2), own // 2
                )
                source = up_own.at[pl.ds(color * (own // 2), own // 2)] if piece == 0 else up.place(
                    color, piece
                )
                return pltpu.make_async_copy(source, up_v.at[at], place_sem.at[color, piece])

            def spell():
                for d in range(n_dp):
                    for k in range(4):
                        for r in range(lines):
                            vectors[k : k + 1, pl.ds(d * own + r * 128, 128)] = p_all[
                                d, k * lines + r : k * lines + r + 1, :
                            ]
                    for r in range(unit // 128):
                        line = 9 * lines + z * (unit // 128) + r
                        vectors[4:5, pl.ds(d * unit + r * 128, 128)] = p_all[
                            d, pl.ds(line, 1), :
                        ]

            def norm(shard):
                block = 32

                def step(i, carry):
                    at = tile(i, block)
                    row = x_all[shard, at, :].astype(f32)
                    center = row - jnp.mean(row, axis=1, keepdims=True)
                    factor = lax.rsqrt(
                        jnp.mean(center * center, axis=1, keepdims=True) + epsilon
                    )
                    normed = center * factor
                    to = pl.ds(pl.multiple_of(shard * rows + i * block, block), block)
                    attn_in[to, :] = (normed * vectors[0:1, :width] + vectors[1:2, :width]).astype(
                        bf16
                    )
                    mlp_in[to, :] = (normed * vectors[2:3, :width] + vectors[3:4, :width]).astype(
                        bf16
                    )
                    return carry

                lax.fori_loop(0, rows // block, step, 0)

            def inner_tile(j):
                at = tile(j, 256)
                inner = dot(mlp_in[...], up_v[:, at], ((1,), (0,))) + vectors[4:5, at]
                cumulative = 0.5 * (1.0 + lax.erf(inner * 0.7071067811865476))
                hidden[:, at] = (inner * cumulative).astype(bf16)
                slope[:, at] = (
                    cumulative + inner * jnp.exp(-0.5 * inner * inner) * 0.3989422804014327
                )

            for color in range(2):
                placed(color, 0).start()

        def first():
            direct.receive()
            p_keep.wait()
            x_keep.wait()
            if whole:
                spell()
                norm(z)

        def x_step(k, way, step):
            step()
            if whole:
                chain = chains[0]
                pl.when(chain.has(way, k))(lambda: norm(z - k if way == 0 else z + k))

        events = [(0.3, first)]
        for i, chain in enumerate(chains):
            for at, step in enumerate(chain.steps()):
                k, way = at // 2 + 1, at % 2
                if i == 0:
                    events.append((k + 0.1, functools.partial(x_step, k, way, step)))
                else:
                    events.append((k + 0.11, step))

        def down_begin():
            loads[-1].wait()
            down.begin()
            down_keep.start()
            scatter.begin()

        events.append((0.1, down_begin))
        for i, spread in enumerate((up, down)):
            pieces = [piece for pair in zip(*spread.arrivals()) for piece in pair]
            for at, (piece, step) in enumerate(zip(pieces, spread.steps())):
                color = at % 2
                order = spread.orders[color]
                chips = piece & ~1
                time = 3 if chips.bit_count() > 1 else 1 + (chips != order[0]) if chips else 0.5

                def run(step=step, color=color, piece=piece, first=i == 0):
                    step()
                    if first and whole:
                        placed(color, piece).start()

                events.append((chips.bit_count() + 0.2 + 0.1 * i + 0.5 * (piece & 1), run))
        events.sort(key=lambda event: event[0])
        early = [event for time, event in events if time <= 3.25]
        late = [event for time, event in events if time > 3.25]
        in_turn(early)
        if whole:
            for color in range(2):
                for piece in range(n_dp):
                    placed(color, piece).wait()
            woven(late, inner_tile, units // 256)
        else:
            in_turn(late)
        for keep in (c_keep, up_keep, down_keep):
            keep.wait()
        for part in (*chains, up, down, direct, scatter):
            part.finish()

    outs = [
        jax.ShapeDtypeStruct((n_seq, rows, width), x.dtype),
        jax.ShapeDtypeStruct((n_seq, rows, width), x.dtype),
        jax.ShapeDtypeStruct((n_dp, *params.shape), params.dtype),
        jax.ShapeDtypeStruct((n_dp, own, units), w_up.dtype),
        jax.ShapeDtypeStruct((n_dp, unit, width), w_down.dtype),
        jax.ShapeDtypeStruct((owners, own // n_dp, width), w_out.dtype),
    ]
    specs = [INSIDE, ANYWHERE, INSIDE, ANYWHERE, ANYWHERE, ANYWHERE]
    scratch = [
        pltpu.VMEM((own, units), w_up.dtype),
        pltpu.VMEM((unit, width), w_down.dtype),
        pltpu.SemaphoreType.DMA((n_dp + 1,)),
        pltpu.SemaphoreType.DMA((5,)),
    ]
    if whole:
        outs += [
            jax.ShapeDtypeStruct((length, width), bf16),
            jax.ShapeDtypeStruct((length, width), bf16),
            jax.ShapeDtypeStruct((length, units), bf16),
            jax.ShapeDtypeStruct((length, units), f32),
        ]
        specs += [INSIDE] * 4
        scratch += [
            pltpu.VMEM((width, units), bf16),
            pltpu.VMEM((8, max(width, units)), f32),
            pltpu.SemaphoreType.DMA((2, n_dp)),
        ]
    return remote_call(
        0,
        body,
        outs,
        specs,
        [INSIDE] * 3 + [ANYWHERE] * 3,
        scratch
        + Chain.sems(n_seq) * 2
        + Spread.sems(n_dp) * 2
        + Direct.sems(n_dp)
        + Scatter.sems(n_dp, owners),
        (x, c, params, w_up, w_down, w_out),
    )


def maker(left, turned, right, columns):
    block = turned.shape[0]
    rows = block // 2

    def make(chip, store):
        turned[...] = left[:, tile(chip, block)].astype(jnp.float32).T.astype(turned.dtype)

        def step(j, carry):
            at = tile(j, columns)
            values = dot(turned[...], right[:, at], ((1,), (0,)))
            for core in range(2):
                store(core, at, values[core * rows : (core + 1) * rows])
            return carry

        lax.fori_loop(0, right.shape[1] // columns, step, 0)

    return make


def mixed(*lists):
    lists = [list(items) for items in lists]
    result = []
    while any(lists):
        for items in lists:
            if items:
                result.append(items.pop(0))
    return result


def down_step(n_dp, hidden, c, slope, down_w):
    f32, bf16 = jnp.float32, jnp.bfloat16
    length, units = hidden.shape
    width = c.shape[1]
    half = units // n_dp // 2

    def body(*refs):
        ins, outs, (dw, slopes, turned, load_sem), scratch = take(refs, 4, 4, 4, 100)
        h_ref, c_ref, s_ref, dw_ref = ins
        sum_ref, grad_ref, bias_ref, mlp_ref = outs
        me, z = lax.axis_index("dp"), lax.axis_index("seq")
        loads = load_all([(dw_ref, dw), (s_ref, slopes)], load_sem)
        greet(n_dp, 1, me, z)
        reduce = Reduce(
            n_dp, me, None, sum_ref, scratch, make=maker(h_ref, turned, c_ref, min(512, width))
        )

        def compute(j):
            at = tile(j, 256)
            grad = dot(c_ref[...], dw[at, :], ((1,), (1,))) * slopes[:, at]
            bias_ref[:, at] = jnp.sum(grad, axis=0, keepdims=True)
            grad_ref[:, at] = grad.astype(bf16)

        def compute_out(j):
            at = tile(j, 256)
            mlp_ref[:, at] = dot(h_ref[...], dw[:, at], ((1,), (0,)))

        turns = list(reduce.steps())
        in_turn(turns[:n_dp])
        for load in loads:
            load.wait()
        early = n_dp // 2
        woven(turns[n_dp : n_dp + early], compute, units // 256, first=units // 512)
        woven(turns[n_dp + early :], compute_out, width // 256, first=width // 512)
        reduce.finish()

    return remote_call(
        1,
        body,
        [
            jax.ShapeDtypeStruct((units // n_dp, width), bf16),
            jax.ShapeDtypeStruct((length, units), bf16),
            jax.ShapeDtypeStruct((1, units), f32),
            jax.ShapeDtypeStruct((length, width), f32),
        ],
        [INSIDE] * 4,
        [INSIDE] * 2 + [ANYWHERE] * 2,
        [
            pltpu.VMEM((units, width), bf16),
            pltpu.VMEM((length, units), f32),
            pltpu.VMEM((4 * half, length), bf16),
            pltpu.SemaphoreType.DMA((2,)),
        ]
        + Reduce.scratch(n_dp, half, width, bf16, made=True),
        (hidden, c, slope, down_w),
    )


def up_step(n_dp, n_seq, left, right, weights, out_own, w_qkv):
    f32, bf16 = jnp.float32, jnp.bfloat16
    length, rows = left.shape
    cols = right.shape[1]
    half = rows // n_dp // 2
    own = w_qkv.shape[0]
    part = H // n_seq * HD

    def body(*refs):
        ins, outs, own_scratch, sems, sems_qkv, scratch = take(refs, 5, 4, 5, 2, 2, 100)
        l_ref, r_ref, w_ref, out_ref, qkv_ref = ins
        sum_ref, back_ref, out_all, qkv_all = outs
        w, turned, qkv_own, load_sem, keep_sem = own_scratch
        me, z = lax.axis_index("dp"), lax.axis_index("seq")
        loads = load_all(
            [(w_ref, w)]
            + [
                (
                    qkv_ref.at[:, pl.ds(pl.multiple_of(i * H * HD + z * part, HD), part)],
                    qkv_own.at[:, pl.ds(i * part, part)],
                )
                for i in range(3)
            ],
            load_sem,
        )
        greet(n_dp, 1, me, z)
        reduce = Reduce(
            n_dp, me, None, sum_ref, scratch, make=maker(l_ref, turned, r_ref, min(512, cols))
        )
        out = Spread(n_dp, me, out_ref, out_all, sems)
        qkv = Spread(n_dp, me, qkv_own, qkv_all, sems_qkv)
        keep = pltpu.make_async_copy(out_ref, out_all.at[me], keep_sem.at[0])
        keep_qkv = pltpu.make_async_copy(qkv_own, qkv_all.at[me], keep_sem.at[1])

        def compute(j):
            at = tile(j, 256)
            back_ref[:, at] = dot(r_ref[...], w[at, :], ((1,), (1,)))

        for load in loads[1:]:
            load.wait()
        qkv.begin()
        out.begin()
        keep_qkv.start()
        keep.start()
        turns = list(reduce.steps())
        in_turn(turns[:n_dp])
        loads[0].wait()
        woven(mixed(turns[n_dp:], qkv.steps(), out.steps()), compute, rows // 256)
        keep_qkv.wait()
        keep.wait()
        for one in (reduce, qkv, out):
            one.finish()

    return remote_call(
        2,
        body,
        [
            jax.ShapeDtypeStruct((rows // n_dp, cols), bf16),
            jax.ShapeDtypeStruct((length, rows), f32),
            jax.ShapeDtypeStruct((n_dp, *out_own.shape), bf16),
            jax.ShapeDtypeStruct((n_dp, own, 3 * part), bf16),
        ],
        [INSIDE] * 2 + [ANYWHERE] * 2,
        [INSIDE] * 2 + [ANYWHERE, INSIDE, ANYWHERE],
        [
            pltpu.VMEM((rows, cols), bf16),
            pltpu.VMEM((4 * half, length), bf16),
            pltpu.VMEM((own, 3 * part), bf16),
            pltpu.SemaphoreType.DMA((4,)),
            pltpu.SemaphoreType.DMA((2,)),
        ]
        + Spread.sems(n_dp) * 2
        + Reduce.scratch(n_dp, half, cols, bf16, made=True),
        (left, right, weights, out_own, w_qkv),
    )


def attention_step(n_dp, n_seq, left, right, weights, out_grad):
    f32, bf16 = jnp.float32, jnp.bfloat16
    length, rows = left.shape
    cols = right.shape[1]
    half = rows // n_dp // 2
    owners = n_dp // n_seq
    own, width = rows // n_dp, out_grad.shape[1]
    size = 2 + 3 + 3 * (bits_of(n_dp) - 1)

    def body(*refs):
        ins, outs, (w, turned, load_sem), first, second = take(refs, 4, 3, 3, size, size)
        l_ref, r_ref, w_ref, g_ref = ins
        sum_ref, back_ref, out_sum = outs
        me, z = lax.axis_index("dp"), lax.axis_index("seq")
        loads = load_all([(w_ref, w)], load_sem)
        greet(n_dp, 1, me, z)
        out = Reduce(
            n_dp,
            me,
            g_ref,
            out_sum,
            first,
            rows_at=lambda dest: 2 * (dest % owners),
            held_by=lambda dest: dest // owners == z,
        )
        reduce = Reduce(
            n_dp, me, None, sum_ref, second, make=maker(l_ref, turned, r_ref, min(512, cols))
        )

        def compute(j):
            at = tile(j, 256)
            back_ref[:, at] = dot(r_ref[...], w[at, :], ((1,), (1,)))

        out.begin()
        turns, out_turns = list(reduce.steps()), list(out.steps())
        in_turn(mixed(turns[:n_dp], out_turns[: n_dp // 2]))
        loads[0].wait()
        woven(mixed(turns[n_dp:], out_turns[n_dp // 2 :]), compute, rows // 256)
        for one in (out, reduce):
            one.finish()

    return remote_call(
        3,
        body,
        [
            jax.ShapeDtypeStruct((own, cols), bf16),
            jax.ShapeDtypeStruct((length, rows), f32),
            jax.ShapeDtypeStruct((own, width), bf16),
        ],
        [INSIDE] * 3,
        [INSIDE] * 2 + [ANYWHERE] * 2,
        [
            pltpu.VMEM((rows, cols), bf16),
            pltpu.VMEM((4 * half, length), bf16),
            pltpu.SemaphoreType.DMA((1,)),
        ]
        + Reduce.scratch(n_dp, own // 2, width, bf16)
        + Reduce.scratch(n_dp, half, cols, bf16, made=True),
        (left, right, weights, out_grad),
    )


def attend(attn_in, triple_w, triple_b, out_w, c, mlp_out, cosine, sine):
    f32, bf16 = jnp.float32, jnp.bfloat16
    length, width = attn_in.shape
    part = triple_w.shape[1] // 3
    heads = part // HD
    scale = HD ** (-0.5)

    def body(a_ref, tb_ref, cos_ref, sin_ref, c_ref, ow_hbm, tw_hbm, mlp_hbm, *rest):
        grad_ref, bias_ref, merged_ref, ahead_ref, tw, ow_ref, mlp, triple, sems = rest
        n_dp, owners, piece, _ = ow_hbm.shape
        loads = load_all(
            [(tw_hbm, tw), (mlp_hbm, mlp)]
            + [
                (
                    ow_hbm.at[d, slot],
                    ow_ref.at[pl.ds((slot * n_dp + d) * piece, piece)],
                )
                for d in range(n_dp)
                for slot in range(owners)
            ],
            sems,
        )
        lanes = lax.broadcasted_iota(jnp.int32, (length, 128), 1)

        def turned(values, direction):
            head = values[:, :128]
            swapped = jnp.where(
                lanes < ROT // 2,
                pltpu.roll(head, 128 - ROT // 2, 1),
                pltpu.roll(head, ROT // 2, 1),
            )
            head = head * cos_ref[...] + direction * swapped * sin_ref[...]
            return jnp.concatenate([head, values[:, 128:]], axis=1)

        rows = lax.broadcasted_iota(jnp.int32, (length, length), 0)
        cols = lax.broadcasted_iota(jnp.int32, (length, length), 1)
        loads[0].wait()

        def project(j, carry):
            at = tile(j, HD)
            triple[:, at] = dot(a_ref[...], tw[:, at], ((1,), (0,))) + tb_ref[:, at]
            return carry

        lax.fori_loop(0, 3 * heads, project, 0)
        for load in loads[2:]:
            load.wait()

        def head(h, carry):
            at = [tile(i * heads + h, HD) for i in range(3)]
            q = turned(triple[:, at[0]], 1.0).astype(bf16)
            k = turned(triple[:, at[1]], 1.0).astype(bf16)
            v = triple[:, at[2]].astype(bf16)
            scores = jnp.where(cols <= rows, dot(q, k, ((1,), (1,))) * scale, masked_fill)
            top = jnp.max(scores, axis=1, keepdims=True)
            logsum = top + jnp.log(jnp.sum(jnp.exp(scores - top), axis=1, keepdims=True))
            probs_f = jnp.exp(scores - logsum)
            probs = probs_f.astype(bf16)
            context = dot(probs, v, ((1,), (0,))).astype(bf16)
            merged_ref[:, at[0]] = context
            context_grad = dot(c_ref[...], ow_ref[at[0], :], ((1,), (1,))).astype(bf16)
            delta = jnp.sum(context_grad.astype(f32) * context.astype(f32), axis=1, keepdims=True)
            prob_grad = dot(context_grad, v, ((1,), (1,)))
            score_grad = probs_f * (prob_grad - delta) * scale
            score_grad_b = score_grad.astype(bf16)
            query_grad = dot(score_grad_b, k, ((1,), (0,))).astype(bf16).astype(f32)
            key_grad = (
                dot(score_grad_b.astype(f32).T.astype(bf16), q, ((1,), (0,)))
                .astype(bf16)
                .astype(f32)
            )
            value_grad = (
                dot(probs.astype(f32).T.astype(bf16), context_grad, ((1,), (0,)))
                .astype(bf16)
                .astype(f32)
            )
            for where, grad in zip(
                at, (turned(query_grad, -1.0), turned(key_grad, -1.0), value_grad)
            ):
                grad_ref[:, where] = grad.astype(bf16)
                bias_ref[:, where] = jnp.sum(grad, axis=0, keepdims=True)
            return carry

        lax.fori_loop(0, heads, head, 0)
        loads[1].wait()

        def join(j, carry):
            at = tile(j, 256)
            total = dot(merged_ref[...], ow_ref[:, at], ((1,), (0,))) + mlp[:, at]
            ahead_ref[:, at] = total.astype(bf16)
            return carry

        lax.fori_loop(0, width // 256, join, 0)

    return pl.pallas_call(
        body,
        out_shape=(
            jax.ShapeDtypeStruct((length, 3 * part), bf16),
            jax.ShapeDtypeStruct((1, 3 * part), f32),
            jax.ShapeDtypeStruct((length, part), bf16),
            jax.ShapeDtypeStruct((length, width), bf16),
        ),
        in_specs=[INSIDE] * 5 + [ANYWHERE] * 3,
        out_specs=(INSIDE,) * 4,
        scratch_shapes=[
            pltpu.VMEM((width, 3 * part), bf16),
            pltpu.VMEM((part, width), bf16),
            pltpu.VMEM((length, width), f32),
            pltpu.VMEM((length, 3 * part), f32),
            pltpu.SemaphoreType.DMA((2 + out_w.shape[0] * out_w.shape[1],)),
        ],
        cost_estimate=pl.CostEstimate(
            flops=20_000_000_000, bytes_accessed=30_000_000, transcendentals=0
        ),
        name="attend",
    )(attn_in, triple_b, cosine, sine, c, out_w, triple_w, mlp_out)


def last_step(n_dp, n_seq, qkv_sum, out_sum, small, ahead, back):
    f32, bf16 = jnp.float32, jnp.bfloat16
    rows, width = back.shape[0] // n_seq, back.shape[1]
    owners = n_dp // n_seq
    few = small.shape[0] // n_dp
    pieces = 4
    size = 2 + 3 + 3 * (bits_of(n_dp) - 1)

    def body(*refs):
        ins, outs, (small_sum, keep_sem), sq, so, ss, a, b, scratch = take(
            refs, 5, 5, 2, 2, 2, 2, 4, 4, size
        )
        q_ref, o_ref, s_ref, a_ref, b_ref = ins
        q_out, o_out, s_out, a_out, b_out = outs
        me, z = lax.axis_index("dp"), lax.axis_index("seq")
        greet(n_dp, n_seq, me, z)
        chain = Chain(n_seq, z, q_ref, q_out, sq)
        little = Reduce(n_dp, me, s_ref, small_sum, scratch)
        tiny = Chain(n_seq, z, small_sum, s_out, ss)
        one = Settle(n_seq, z, a_ref, a_out, a)
        two = Settle(n_seq, z, b_ref, b_out, b)
        cast = Cast(n_seq, z, me // owners, o_ref, o_out, so, pieces)
        chain.begin()
        keep = pltpu.make_async_copy(q_ref, q_out.at[z], keep_sem.at[0])
        keep.start()
        little.begin()
        in_turn(little.steps())
        tiny.begin()
        keep_small = pltpu.make_async_copy(small_sum, s_out.at[z], keep_sem.at[1])
        keep_small.start()
        one.begin()
        cast.begin()
        two.begin()

        events = []
        for at, step in enumerate(chain.steps()):
            events.append((1.5 * (at // 2 + 1), step))
        for at, step in enumerate(tiny.steps()):
            events.append((1.5 * (at // 2 + 1) + 0.1, step))
        for start, settle in ((2.4, one), (7.4, two)):
            steps = list(settle.steps())
            for at, step in enumerate(steps[:-3]):
                events.append((start + at // 2, step))
            events.append((start - 2, steps[-3]))
            for step in steps[-2:]:
                events.append((start + n_seq - 2, step))
        for at, step in enumerate(cast.steps()):
            events.append((5.2 + 0.5 * (at // 2), step))
        in_turn([step for _, step in sorted(events, key=lambda event: event[0])])
        keep.wait()
        keep_small.wait()
        for part in (chain, tiny, one, two, cast, little):
            part.finish()

    return remote_call(
        4,
        body,
        [
            jax.ShapeDtypeStruct((n_seq, *qkv_sum.shape), bf16),
            jax.ShapeDtypeStruct(out_sum.shape, bf16),
            jax.ShapeDtypeStruct((n_seq, few, small.shape[1]), f32),
            jax.ShapeDtypeStruct((rows, width), f32),
            jax.ShapeDtypeStruct((rows, width), f32),
        ],
        [ANYWHERE] * 3 + [INSIDE] * 2,
        [INSIDE] * 2 + [ANYWHERE] + [INSIDE] * 2,
        [pltpu.VMEM((few, small.shape[1]), f32), pltpu.SemaphoreType.DMA((2,))]
        + Chain.sems(n_seq)
        + Cast.sems(pieces)
        + Chain.sems(n_seq)
        + Settle.scratch(n_seq, rows, width, bf16) * 2
        + Reduce.scratch(n_dp, few // 2, small.shape[1], f32),
        (
            qkv_sum,
            out_sum,
            small,
            ahead.reshape(n_seq, rows, width),
            back.reshape(n_seq, rows, width),
        ),
    )


def widen_kernel(parts_ref, out_ref):
    count, _, unit = parts_ref.shape
    for s in range(count):
        out_ref[:, s * unit : (s + 1) * unit] = parts_ref[s].astype(jnp.float32)


def widen(parts, blocks):
    n_seq, rows, cols = parts.shape
    unit = cols // blocks
    if unit % 128:
        return (
            parts.reshape(n_seq, rows, blocks, unit)
            .transpose(1, 2, 0, 3)
            .reshape(rows, n_seq * cols)
            .astype(jnp.float32)
        )
    return pl.pallas_call(
        widen_kernel,
        grid=(blocks,),
        out_shape=jax.ShapeDtypeStruct((rows, n_seq * cols), jnp.float32),
        in_specs=[pl.BlockSpec((n_seq, rows, unit), lambda j: (0, 0, j))],
        out_specs=pl.BlockSpec((rows, n_seq * unit), lambda j: (0, j)),
        cost_estimate=pl.CostEstimate(
            flops=0, bytes_accessed=6 * n_seq * rows * cols, transcendentals=0
        ),
        name="widen",
    )(parts)


def held(after, *values):
    return lax.optimization_barrier((*values, after))[:-1]


def normalize(rows):
    center = rows - jnp.mean(rows, axis=-1, keepdims=True)
    factor = lax.rsqrt(jnp.mean(center * center, axis=-1, keepdims=True) + epsilon)
    return center * factor, factor


def angles(positions):
    half = ROT // 2
    freqs = 10000.0 ** (-2.0 * jnp.arange(half).astype(positions.dtype) / ROT)
    theta = positions[:, None] * freqs[None, :]
    return (jnp.cos(theta), jnp.sin(theta))


def gather_seq(shard):
    return lax.all_gather(shard, "seq", axis=0, tiled=False)


def make_local(n_dp, n_seq):
    def local(
        layer_input,
        cotangent,
        ln1_gain,
        ln1_bias,
        w_qkv,
        b_qkv,
        w_out,
        b_out,
        ln2_gain,
        ln2_bias,
        w_up,
        b_up,
        w_down,
        b_down,
    ):
        f32, bf16 = jnp.float32, jnp.bfloat16
        _, tok_local, width = layer_input.shape
        length = tok_local * n_seq
        own = width // n_dp
        ff = w_up.shape[1]
        ff_own = ff // n_dp
        unit = ff_own // n_seq
        heads = H // n_seq
        owners = n_dp // n_seq
        z = lax.axis_index("seq")
        me = lax.axis_index("dp")

        packed = jnp.concatenate(
            [ln1_gain, ln1_bias, ln2_gain, ln2_bias, b_out, b_down, b_qkv, b_up]
        )
        packed = jnp.pad(packed, (0, -packed.shape[0] % 2048)).reshape(-1, 128)
        tokens, incoming, gathered, up_w, down_w, out_own, *made = fetch(
            n_dp,
            n_seq,
            unit,
            layer_input.reshape(tok_local, width),
            cotangent.reshape(tok_local, width),
            packed,
            w_up,
            w_down,
            w_out,
        )
        tokens, incoming = tokens.reshape(length, width), incoming.reshape(length, width)
        gathered = gathered.reshape(n_dp, -1)
        up_w = up_w.reshape(width, n_dp * unit)
        down_w = down_w.reshape(n_dp * unit, width)

        gain_one, shift_one, gain_two, shift_two, out_b, down_b = (
            gathered[:, k * own : (k + 1) * own].reshape(width) for k in range(6)
        )
        base = 6 * own
        triple_b = lax.dynamic_slice_in_dim(
            gathered[:, base : base + 3 * own].reshape(3, H, HD), z * heads, heads, 1
        ).reshape(3 * heads * HD)
        up_b = lax.dynamic_index_in_dim(
            gathered[:, base + 3 * own : base + 3 * own + ff_own].reshape(n_dp, n_seq, unit),
            z,
            1,
            keepdims=False,
        ).reshape(n_dp * unit)

        if made:
            mlp_in, attn_in, hidden, slope = made
        else:
            normed, _ = normalize(tokens.astype(f32))
            mlp_in = (normed * gain_two + shift_two).astype(bf16)
            attn_in = (normed * gain_one + shift_one).astype(bf16)
            inner = dot(mlp_in, up_w, ((1,), (0,))) + up_b
            cumulative = 0.5 * (1.0 + lax.erf(inner * 0.7071067811865476))
            hidden = (inner * cumulative).astype(bf16)
            slope = cumulative + inner * jnp.exp(-0.5 * inner * inner) * 0.3989422804014327
        down_sum, inner_grad_b, b_up_grad, mlp_out = down_step(
            n_dp, hidden, incoming, slope, down_w
        )
        down_part = gather_seq(down_sum)
        up_sum, mlp_in_grad, out_w, triple_w = up_step(
            n_dp,
            n_seq,
            mlp_in,
            inner_grad_b,
            up_w,
            out_own.reshape(-1, width),
            w_qkv,
        )
        up_part = gather_seq(up_sum)
        out_w = out_w.reshape(n_dp, owners, own // n_dp, width)
        triple_w = triple_w.reshape(width, 3 * heads * HD)

        (tokens,) = held(up_sum, tokens)
        normed, _ = normalize(tokens.astype(f32))
        ln2_gain_grad = jnp.sum(mlp_in_grad * normed, axis=0)
        ln2_bias_grad = jnp.sum(mlp_in_grad, axis=0)
        cosine, sine = angles(jnp.arange(length, dtype=jnp.int32).astype(f32))
        still = jnp.zeros((length, 128 - ROT), f32)
        triple_grad_b, b_qkv_grad, merged, ahead = attend(
            attn_in,
            triple_w,
            triple_b.reshape(1, -1),
            out_w,
            incoming,
            mlp_out,
            jnp.concatenate([cosine, cosine, still + 1.0], axis=1),
            jnp.concatenate([-sine, sine, still], axis=1),
        )
        out_grad = dot(merged, incoming, ((0,), (0,))).astype(bf16)
        qkv_sum, attn_in_grad, out_sum = attention_step(
            n_dp, n_seq, attn_in, triple_grad_b, triple_w, out_grad
        )
        ln1_gain_grad = jnp.sum(attn_in_grad * normed, axis=0)
        ln1_bias_grad = jnp.sum(attn_in_grad, axis=0)

        rows = layer_input.reshape(tok_local, width).astype(f32)
        grad_rows = cotangent.reshape(tok_local, width).astype(f32)
        here = jnp.arange(n_seq) == z
        b_up_wide = jnp.where(
            here[None, :, None], b_up_grad.reshape(n_dp, 1, unit), 0.0
        ).reshape(n_dp, ff_own)
        b_qkv_wide = jnp.where(
            here[None, :, None], b_qkv_grad.reshape(3, 1, heads * HD), 0.0
        ).reshape(n_dp, 3 * own)
        b_down_grad = jnp.sum(grad_rows, axis=0)
        small = jnp.concatenate(
            [
                ln1_gain_grad.reshape(n_dp, own),
                ln1_bias_grad.reshape(n_dp, own),
                ln2_gain_grad.reshape(n_dp, own),
                ln2_bias_grad.reshape(n_dp, own),
                b_down_grad.reshape(n_dp, own),
                b_qkv_wide,
                b_up_wide,
            ],
            axis=1,
        )
        small_len = small.shape[1]
        small = jnp.pad(small, ((0, 0), (0, -small_len % 4096))).reshape(-1, 256)

        back = attn_in_grad * gain_one + mlp_in_grad * gain_two
        qkv_part, out_cast, small_all, ahead, scaled = last_step(
            n_dp, n_seq, qkv_sum, out_sum, small, ahead, back.astype(bf16)
        )
        output = rows + (out_b + down_b) + ahead
        normed_own, factor_own = normalize(rows)
        input_grad = grad_rows + factor_own * (
            scaled
            - jnp.mean(scaled, axis=-1, keepdims=True)
            - normed_own * jnp.mean(scaled * normed_own, axis=-1, keepdims=True)
        )
        mine = jnp.sum(small_all, axis=0).reshape(-1)
        g1, s1, g2, s2, bd = (mine[k * own : (k + 1) * own] for k in range(5))
        bq = mine[5 * own : 8 * own]
        bu = mine[8 * own : small_len]
        out_full = jnp.where(me // owners == z, out_sum, out_cast).astype(f32)
        down_full = down_part.reshape(ff_own, width).astype(f32)
        up_full = widen(up_part, n_dp)
        qkv_full = widen(qkv_part, 3)

        return (
            output.reshape(layer_input.shape),
            input_grad.reshape(layer_input.shape),
            g1,
            s1,
            qkv_full,
            bq,
            out_full,
            bd,
            g2,
            s2,
            up_full,
            bu,
            down_full,
            bd,
        )

    return local


def solution(mesh):
    vector, matrix, tokens = P("dp"), P("dp", None), P("dp", "seq", None)
    specs = (
        tokens,
        tokens,
        vector,
        vector,
        matrix,
        vector,
        matrix,
        vector,
        vector,
        vector,
        matrix,
        vector,
        matrix,
        vector,
    )
    local = make_local(mesh.shape["dp"], mesh.shape["seq"])

    return jax.shard_map(local, mesh=mesh, in_specs=specs, out_specs=specs, check_vma=False)
```

```python
import functools

import jax
import jax.numpy as jnp
from jax import lax
from jax.experimental import pallas as pl
from jax.experimental.pallas import tpu as pltpu
from jax.sharding import PartitionSpec as P


H = 8
HD = 256
ROT = 64

epsilon = 1e-05
masked_fill = -1e30

MESH = pl.DeviceIdType.MESH
ANYWHERE = pl.BlockSpec(memory_space=pl.ANY)
INSIDE = pl.BlockSpec(memory_space=pltpu.VMEM)


def dot(a, b, contract):
    return lax.dot_general(a, b, (contract, ((), ())), preferred_element_type=jnp.float32)


def tile(index, size):
    start = index * size
    return pl.ds(start if isinstance(start, int) else pl.multiple_of(start, size), size)


def guarded(condition, body):
    if condition is None:
        body()
    else:
        pl.when(condition)(body)


def bits_of(n):
    return n.bit_length() - 1


def flipped(me, mask):
    for k in range(mask.bit_length()):
        if mask >> k & 1:
            me = me + (1 << k) * (1 - 2 * ((me // (1 << k)) % 2))
    return me


def chip_orders(n):
    chips = [1 << k for k in range(1, bits_of(n))]
    return chips, chips[1:] + chips[:1]


def greet(n_dp, n_seq, me, z, everyone=False):
    barrier = pltpu.get_barrier_semaphore()
    masks = range(1, n_dp) if everyone else [1 << k for k in range(bits_of(n_dp))]
    for mask in masks:
        pl.semaphore_signal(
            barrier, inc=1, device_id={"dp": flipped(me, mask)}, device_id_type=MESH
        )
    peers = len(masks)
    if n_seq > 1:

        @pl.when(z > 0)
        def _():
            pl.semaphore_signal(barrier, inc=1, device_id={"seq": z - 1}, device_id_type=MESH)

        @pl.when(z < n_seq - 1)
        def _():
            pl.semaphore_signal(barrier, inc=1, device_id={"seq": z + 1}, device_id_type=MESH)

        peers = peers + (z + n_seq - 1) // n_seq + (2 * n_seq - 2 - z) // n_seq
    pl.semaphore_wait(barrier, peers)


def in_turn(*lists):
    lists = [list(steps) for steps in lists]
    while any(lists):
        for steps in lists:
            if steps:
                steps.pop(0)()


class Spread:
    def __init__(self, n_dp, me, own, out, sems, held_by=None, slot=None):
        self.n_dp, self.me, self.own, self.out = n_dp, me, own, out
        self.send_sem, self.recv_sem = sems
        self.half = own.shape[0] // 2
        self.orders = [list(order) + [1] for order in chip_orders(n_dp)]
        self.held_by = held_by or (lambda owner: None)
        self.slot = slot or (lambda owner: owner)

    @staticmethod
    def sems(n_dp):
        return [pltpu.SemaphoreType.DMA((2, n_dp)), pltpu.SemaphoreType.DMA((2, n_dp))]

    def place(self, color, piece):
        owner = flipped(self.me, piece)
        return self.out.at[self.slot(owner), pl.ds(color * self.half, self.half)]

    def copy(self, color, piece, bit, arrived=False):
        if arrived or piece:
            source = self.place(color, piece)
        else:
            source = self.own.at[pl.ds(color * self.half, self.half)]
        key = piece if arrived else piece | bit
        return pltpu.make_async_remote_copy(
            src_ref=source,
            dst_ref=self.place(color, piece),
            send_sem=self.send_sem.at[color, key],
            recv_sem=self.recv_sem.at[color, key],
            device_id={"dp": flipped(self.me, bit)},
            device_id_type=MESH,
        )

    def later(self, color, piece):
        order = self.orders[color]
        last = max((order.index(b) for b in order if piece & b), default=-1)
        return order[last + 1 :]

    def start(self, color, piece=0):
        def body():
            for bit in self.later(color, piece):
                self.copy(color, piece, bit).start()

        guarded(self.held_by(flipped(self.me, piece)), body)

    def begin(self):
        for color in range(2):
            self.start(color)

    def receive(self, color, piece):
        order = self.orders[color]
        bit = order[max(order.index(b) for b in order if piece & b)]

        def body():
            self.copy(color, piece, bit, arrived=True).wait_recv()

        guarded(self.held_by(flipped(self.me, piece)), body)

    def arrivals(self):
        lists = []
        for order in self.orders:
            pieces = [0]
            for bit in order:
                pieces += [p | bit for p in pieces]
            lists.append(pieces[1:])
        return lists

    def steps(self):
        for pair in zip(*self.arrivals()):
            for color, piece in enumerate(pair):

                def step(color=color, piece=piece):
                    self.receive(color, piece)
                    self.start(color, piece)

                yield step

    def finish(self):
        for color in range(2):
            for piece in range(self.n_dp):

                def body():
                    for bit in self.later(color, piece):
                        self.copy(color, piece, bit).wait_send()

                guarded(self.held_by(flipped(self.me, piece)), body)


class Chain:
    def __init__(self, n_seq, z, own, out, sems):
        self.n_seq, self.z, self.own, self.out = n_seq, z, own, out
        self.send_sem, self.recv_sem = sems

    @staticmethod
    def sems(n_seq):
        return [pltpu.SemaphoreType.DMA((2, n_seq)), pltpu.SemaphoreType.DMA((2, n_seq))]

    def copy(self, way, k, arrived=False):
        shard = self.z - k if way == 0 else self.z + k
        source = self.own if k == 0 else self.out.at[shard]
        key = k - 1 if arrived else k
        return pltpu.make_async_remote_copy(
            src_ref=source,
            dst_ref=self.out.at[shard],
            send_sem=self.send_sem.at[way, key],
            recv_sem=self.recv_sem.at[way, key],
            device_id={"seq": self.z + 1 if (way == 0) != arrived else self.z - 1},
            device_id_type=MESH,
        )

    def has(self, way, k):
        return self.z >= k if way == 0 else self.z + k <= self.n_seq - 1

    def more(self, way):
        return self.z < self.n_seq - 1 if way == 0 else self.z > 0

    def sends(self, way, k):
        return jnp.logical_and(self.has(way, k), self.more(way))

    def begin(self):
        for way in range(2):
            pl.when(self.sends(way, 0))(lambda: self.copy(way, 0).start())

    def steps(self):
        for k in range(1, self.n_seq):
            for way in range(2):

                def step(k=k, way=way):
                    pl.when(self.has(way, k))(lambda: self.copy(way, k, True).wait_recv())
                    if k < self.n_seq - 1:
                        pl.when(self.sends(way, k))(lambda: self.copy(way, k).start())

                yield step

    def finish(self):
        for k in range(self.n_seq - 1):
            for way in range(2):
                pl.when(self.sends(way, k))(lambda: self.copy(way, k).wait_send())


class Cast:
    def __init__(self, n_seq, z, origin, own, out, sems, pieces):
        self.n_seq, self.z, self.origin, self.own, self.out = n_seq, z, origin, own, out
        self.send_sem, self.recv_sem = sems
        self.pieces, self.rows = pieces, own.shape[0] // pieces

    @staticmethod
    def sems(pieces):
        return [pltpu.SemaphoreType.DMA((2, pieces)), pltpu.SemaphoreType.DMA((2, pieces))]

    def copy(self, way, piece, source, arrived=False):
        at = pl.ds(piece * self.rows, self.rows)
        return pltpu.make_async_remote_copy(
            src_ref=source.at[at],
            dst_ref=self.out.at[at],
            send_sem=self.send_sem.at[way, piece],
            recv_sem=self.recv_sem.at[way, piece],
            device_id={"seq": self.z + 1 if (way == 0) != arrived else self.z - 1},
            device_id_type=MESH,
        )

    def more(self, way):
        return self.z < self.n_seq - 1 if way == 0 else self.z > 0

    def sends(self, way, first):
        if first:
            here = self.z == self.origin
        else:
            here = self.z > self.origin if way == 0 else self.z < self.origin
        return jnp.logical_and(here, self.more(way))

    def begin(self):
        for piece in range(self.pieces):
            for way in range(2):
                pl.when(self.sends(way, True))(lambda: self.copy(way, piece, self.own).start())

    def steps(self):
        for piece in range(self.pieces):
            for way in range(2):

                def step(piece=piece, way=way):
                    got = self.z > self.origin if way == 0 else self.z < self.origin
                    pl.when(got)(lambda: self.copy(way, piece, self.out, True).wait_recv())
                    pl.when(self.sends(way, False))(
                        lambda: self.copy(way, piece, self.out).start()
                    )

                yield step

    def finish(self):
        for piece in range(self.pieces):
            for way in range(2):
                for first in (True, False):
                    pl.when(self.sends(way, first))(
                        lambda: self.copy(way, piece, self.out).wait_send()
                    )


class Direct:
    def __init__(self, n_dp, me, own, out, sems):
        self.n_dp, self.me, self.own, self.out = n_dp, me, own, out
        self.send_sem, self.recv_sem = sems

    @staticmethod
    def sems(n_dp):
        return [pltpu.SemaphoreType.DMA((n_dp,)), pltpu.SemaphoreType.DMA((n_dp,))]

    def copy(self, mask, owner):
        return pltpu.make_async_remote_copy(
            src_ref=self.own,
            dst_ref=self.out.at[owner],
            send_sem=self.send_sem.at[mask],
            recv_sem=self.recv_sem.at[mask],
            device_id={"dp": flipped(self.me, mask)},
            device_id_type=MESH,
        )

    def begin(self):
        for mask in range(1, self.n_dp):
            self.copy(mask, self.me).start()

    def receive(self):
        for mask in range(1, self.n_dp):
            self.copy(mask, flipped(self.me, mask)).wait_recv()

    def finish(self):
        for mask in range(1, self.n_dp):
            self.copy(mask, self.me).wait_send()


class Scatter:
    def __init__(self, n_dp, owners, me, z, rows, out, sems):
        self.n_dp, self.owners, self.me, self.z, self.rows, self.out = n_dp, owners, me, z, rows, out
        self.send_sem, self.recv_sem = sems
        self.piece = rows.shape[0] // n_dp

    @staticmethod
    def sems(n_dp, owners):
        return [pltpu.SemaphoreType.DMA((n_dp,)), pltpu.SemaphoreType.DMA((owners,))]

    def source(self, dest):
        return self.rows.at[pl.ds(pl.multiple_of(dest * self.piece, self.piece), self.piece)]

    def copy(self, mask, slot):
        dest = flipped(self.me, mask)
        return pltpu.make_async_remote_copy(
            src_ref=self.source(dest),
            dst_ref=self.out.at[slot],
            send_sem=self.send_sem.at[mask],
            recv_sem=self.recv_sem.at[slot],
            device_id={"dp": dest},
            device_id_type=MESH,
        )

    def keep(self):
        return pltpu.make_async_copy(
            self.source(self.me), self.out.at[self.me % self.owners], self.send_sem.at[0]
        )

    def when(self, body):
        pl.when(self.me // self.owners == self.z)(body)

    def begin(self):
        def body():
            for mask in range(1, self.n_dp):
                self.copy(mask, self.me % self.owners).start()
            self.keep().start()

        self.when(body)

    def finish(self):
        for slot in range(self.owners):
            pl.when(self.z * self.owners + slot != self.me)(
                lambda: self.copy(1, slot).wait_recv()
            )

        def body():
            for mask in range(1, self.n_dp):
                self.copy(mask, self.me % self.owners).wait_send()
            self.keep().wait()

        self.when(body)


class Reduce:
    def __init__(self, n_dp, me, grad, out, scratch, rows_at=None, held_by=None, make=None):
        self.n_dp, self.me, self.grad, self.out = n_dp, me, grad, out
        self.mine, self.first, self.load_sem, self.s0, self.r0, *self.stages = scratch
        self.half = out.shape[0] // 2
        self.orders = chip_orders(n_dp)
        self.rows_at = rows_at or (lambda dest: 2 * dest)
        self.held_by = held_by or (lambda dest: None)
        self.make = make
        self.dests = sorted(range(0, n_dp, 2), key=lambda d: -d.bit_count())

    @staticmethod
    def scratch(n_dp, half, cols, kind, made=False):
        pairs = n_dp // 2
        result = [
            pltpu.VMEM((2 if made else 1, 2, pairs, half, cols), kind),
            pltpu.VMEM((2, pairs, half, cols), kind),
            pltpu.SemaphoreType.DMA((2, pairs)),
            pltpu.SemaphoreType.DMA((2, pairs)),
            pltpu.SemaphoreType.DMA((2, pairs)),
        ]
        for stage in range(bits_of(n_dp) - 1):
            left = pairs >> (stage + 1)
            result += [
                pltpu.VMEM((2, left, half, cols), kind),
                pltpu.SemaphoreType.DMA((2, left)),
                pltpu.SemaphoreType.DMA((2, left)),
            ]
        return result

    def kept(self, color, dest):
        core = self.me % 2 if self.make else 0
        return self.mine.at[core, color, dest // 2]

    def when(self, dest, body):
        guarded(self.held_by(flipped(self.me, dest)), body)

    def source(self, color, dest):
        start = (self.rows_at(flipped(self.me, dest)) + color) * self.half
        return self.grad.at[pl.ds(pl.multiple_of(start, self.half), self.half)]

    def core_copy(self, color, dest):
        if self.make:
            source = self.mine.at[1 - self.me % 2, color, dest // 2]
        else:
            source = self.source(color, dest | 1)
        return pltpu.make_async_remote_copy(
            src_ref=source,
            dst_ref=self.first.at[color, dest // 2],
            send_sem=self.s0.at[color, dest // 2],
            recv_sem=self.r0.at[color, dest // 2],
            device_id={"dp": flipped(self.me, 1)},
            device_id_type=MESH,
        )

    def own_load(self, color, dest):
        return pltpu.make_async_copy(
            self.source(color, dest), self.kept(color, dest), self.load_sem.at[color, dest // 2]
        )

    def slot(self, color, stage, dest):
        rest = self.orders[color][stage + 1 :]
        return sum(1 << k for k, bit in enumerate(rest) if dest & bit)

    def stage_copy(self, color, stage, dest):
        bit = self.orders[color][stage]
        land, ss, rr = self.stages[3 * stage : 3 * stage + 3]
        at = self.slot(color, stage, dest & ~bit)
        return pltpu.make_async_remote_copy(
            src_ref=self.kept(color, dest),
            dst_ref=land.at[color, at],
            send_sem=ss.at[color, at],
            recv_sem=rr.at[color, at],
            device_id={"dp": flipped(self.me, bit)},
            device_id_type=MESH,
        )

    def add(self, color, dest, other, target):
        block = min(16, self.half)
        kept = self.kept(color, dest)

        def body(step, carry):
            at = pl.ds(pl.multiple_of(step * block, block), block)
            total = kept[at, :].astype(jnp.float32) + other[at, :].astype(jnp.float32)
            target[at, :] = total.astype(target.dtype)
            return carry

        lax.fori_loop(0, self.half // block, body, 0)

    def begin(self):
        if not self.make:
            for dest in self.dests:
                self.give(dest)

    def give(self, dest):
        if self.make:
            half = self.half

            def store(core, columns, values):
                for color in range(2):
                    self.mine[core, color, dest // 2, :, columns] = values[
                        color * half : (color + 1) * half
                    ].astype(self.mine.dtype)

            self.make(flipped(self.me, dest) // 2, store)

        def body():
            for color in range(2):
                self.core_copy(color, dest).start()
                if not self.make:
                    self.own_load(color, dest).start()

        self.when(dest, body)

    def meet(self, dest):
        def body():
            for color in range(2):
                self.core_copy(color, dest).wait_recv()
                if not self.make:
                    self.own_load(color, dest).wait()
                self.add(
                    color, dest, self.first.at[color, dest // 2], self.kept(color, dest)
                )
                if dest & self.orders[color][0]:
                    self.stage_copy(color, 0, dest).start()

        self.when(dest, body)

    def merge(self, stage, color, dest):
        order = self.orders[color]

        def body():
            self.stage_copy(color, stage, dest | order[stage]).wait_recv()
            place = self.stages[3 * stage].at[color, self.slot(color, stage, dest)]
            if stage == len(order) - 1:
                self.add(color, dest, place, self.out.at[pl.ds(color * self.half, self.half)])
            else:
                self.add(color, dest, place, self.kept(color, dest))
                if dest & order[stage + 1]:
                    self.stage_copy(color, stage + 1, dest).start()

        self.when(dest, body)

    def steps(self):
        gives = [functools.partial(self.give, dest) for dest in self.dests] if self.make else []
        meets = [functools.partial(self.meet, dest) for dest in self.dests]
        while gives or meets:
            if gives:
                yield gives.pop(0)
            if len(gives) < len(meets) - 1 or not gives:
                yield meets.pop(0)
        for stage in range(len(self.orders[0])):
            for dest in self.dests:
                for color in range(2):
                    if not any(dest & bit for bit in self.orders[color][: stage + 1]):
                        yield functools.partial(self.merge, stage, color, dest)

    def finish(self):
        for dest in self.dests:

            def body():
                for color in range(2):
                    self.core_copy(color, dest).wait_send()

            self.when(dest, body)
            for color in range(2):
                for stage, bit in enumerate(self.orders[color]):
                    if dest & bit and not any(dest & b for b in self.orders[color][:stage]):
                        self.when(
                            dest, lambda: self.stage_copy(color, stage, dest).wait_send()
                        )


class Settle:
    def __init__(self, n_seq, z, partial, out, scratch):
        self.n_seq, self.z, self.partial, self.out = n_seq, z, partial, out
        self.land, self.stage, self.send_sem, self.recv_sem = scratch

    @staticmethod
    def scratch(n_seq, rows, width, kind):
        return [
            pltpu.VMEM((2, n_seq - 1, rows, width), kind),
            pltpu.VMEM((2, n_seq - 2, rows, width), kind),
            pltpu.SemaphoreType.DMA((2, n_seq - 1)),
            pltpu.SemaphoreType.DMA((2, n_seq - 1)),
        ]

    def slab(self, way, k):
        return self.z + k if way == 0 else self.z - k

    def copy(self, way, k, source):
        return pltpu.make_async_remote_copy(
            src_ref=source,
            dst_ref=self.land.at[way, k - 1],
            send_sem=self.send_sem.at[way, k - 1],
            recv_sem=self.recv_sem.at[way, k - 1],
            device_id={"seq": self.z + 1 if way == 0 else self.z - 1},
            device_id_type=MESH,
        )

    def first(self, way):
        return self.z == 0 if way == 0 else self.z == self.n_seq - 1

    def reaches(self, way, k):
        return self.z + k <= self.n_seq - 1 if way == 0 else self.z >= k

    def each(self, body):
        block = 16

        def step(i, carry):
            body(pl.ds(pl.multiple_of(i * block, block), block))
            return carry

        lax.fori_loop(0, self.out.shape[0] // block, step, 0)

    def begin(self):
        for k in range(self.n_seq - 1, 0, -1):
            for way in range(2):
                pl.when(jnp.logical_and(self.first(way), self.reaches(way, k)))(
                    lambda: self.copy(way, k, self.partial.at[self.slab(way, k)]).start()
                )

    def pass_on(self, way, k):
        def body():
            self.copy(way, k + 1, self.land.at[way, k]).wait_recv()

            def add(at):
                total = self.partial[self.slab(way, k), at, :].astype(jnp.float32) + self.land[
                    way, k, at, :
                ].astype(jnp.float32)
                self.stage[way, k - 1, at, :] = total.astype(self.stage.dtype)

            self.each(add)
            self.copy(way, k, self.stage.at[way, k - 1]).start()

        pl.when(jnp.logical_and(jnp.logical_not(self.first(way)), self.reaches(way, k)))(body)

    def keep(self):
        def add(at):
            self.out[at, :] = self.partial[self.z, at, :].astype(jnp.float32)

        self.each(add)

    def close(self, way):
        def body():
            self.copy(way, 1, self.land.at[way, 0]).wait_recv()

            def add(at):
                self.out[at, :] += self.land[way, 0, at, :].astype(jnp.float32)

            self.each(add)

        pl.when(jnp.logical_not(self.first(way)))(body)

    def steps(self):
        for k in range(self.n_seq - 2, 0, -1):
            for way in range(2):
                yield functools.partial(self.pass_on, way, k)
        yield self.keep
        for way in range(2):
            yield functools.partial(self.close, way)

    def finish(self):
        for k in range(self.n_seq - 1, 0, -1):
            for way in range(2):
                pl.when(self.reaches(way, k))(
                    lambda: self.copy(way, k, self.land.at[way, k - 1]).wait_send()
                )


def take(refs, *counts):
    groups, at = [], 0
    for count in counts:
        groups.append(refs[at : at + count])
        at += count
    return groups


def remote_call(ident, body, outs, out_specs, in_specs, scratch, args):
    return pl.pallas_call(
        body,
        out_shape=tuple(outs),
        in_specs=in_specs,
        out_specs=tuple(out_specs),
        scratch_shapes=scratch,
        compiler_params=pltpu.CompilerParams(collective_id=ident, has_side_effects=True),
        cost_estimate=pl.CostEstimate(flops=0, bytes_accessed=100_000_000, transcendentals=0),
    )(*args)


def load_all(pairs, sems):
    loads = [
        pltpu.make_async_copy(source, target, sems.at[i])
        for i, (source, target) in enumerate(pairs)
    ]
    for load in loads:
        load.start()
    return loads


def woven(steps, compute, count, first=0):
    steps = list(steps)

    def body(j, carry):
        compute(j)
        done = 0
        for i in range(first, count):
            upto = len(steps) * (i + 1 - first) // (count - first)
            if upto > done:
                pl.when(j == i)(lambda: [step() for step in steps[done:upto]] and None)
            done = upto
        return carry

    lax.fori_loop(0, count, body, 0)


def fetch(n_dp, n_seq, unit, x, c, params, w_up, w_down, w_out):
    f32, bf16 = jnp.float32, jnp.bfloat16
    rows, width = x.shape
    own = w_up.shape[0]
    units = n_dp * unit
    length = n_seq * rows
    owners = n_dp // n_seq
    lines = own // 128
    whole = unit % 128 == 0 and own % 128 == 0
    if not whole:
        w_up = lax.dynamic_index_in_dim(
            w_up.reshape(own, n_dp, n_seq, unit), lax.axis_index("seq"), 2, keepdims=False
        ).reshape(own, units)
    extra = 4 if whole else 0

    def body(*refs):
        ins, outs, made, own_scratch, inner_scratch, sems = take(
            refs, 6, 6, extra, 4, 3 if whole else 0, 12
        )
        x_ref, c_ref, p_ref, up_ref, down_ref, out_ref = ins
        x_all, c_all, p_all, up_all, down_all, out_piece = outs
        up_own, down_own, load_sem, keep_sem = own_scratch
        me, z = lax.axis_index("dp"), lax.axis_index("seq")
        if whole:
            pairs = [
                (
                    up_ref.at[:, pl.ds(pl.multiple_of((d * n_seq + z) * unit, 128), unit)],
                    up_own.at[:, pl.ds(d * unit, unit)],
                )
                for d in range(n_dp)
            ]
        else:
            pairs = [(up_ref, up_own)]
        loads = load_all([*pairs, (down_ref.at[tile(z, unit)], down_own)], load_sem)
        greet(n_dp, n_seq, me, z, everyone=True)
        chains = [
            Chain(n_seq, z, source, out, sems[2 * i : 2 * i + 2])
            for i, (source, out) in enumerate(((x_ref, x_all), (c_ref, c_all)))
        ]
        up, down = (
            Spread(n_dp, me, source, out, sems[4 + 2 * i : 6 + 2 * i])
            for i, (source, out) in enumerate(((up_own, up_all), (down_own, down_all)))
        )
        direct = Direct(n_dp, me, p_ref, p_all, sems[8:10])
        scatter = Scatter(n_dp, owners, me, z, out_ref, out_piece, sems[10:12])
        direct.begin()
        chains[0].begin()
        chains[1].begin()
        for load in loads[:-1]:
            load.wait()
        up.begin()
        x_keep, c_keep, p_keep, up_keep, down_keep = (
            pltpu.make_async_copy(source, out.at[at], keep_sem.at[i])
            for i, (source, out, at) in enumerate(
                (
                    (x_ref, x_all, z),
                    (c_ref, c_all, z),
                    (p_ref, p_all, me),
                    (up_own, up_all, me),
                    (down_own, down_all, me),
                )
            )
        )
        keeps = (x_keep, c_keep, p_keep, up_keep, down_keep)
        for keep in keeps[:4]:
            keep.start()

        if whole:
            mlp_in, attn_in, hidden, slope = made
            up_v, vectors, place_sem = inner_scratch

            def placed(color, piece):
                owner = flipped(me, piece)
                at = pl.ds(
                    pl.multiple_of(owner * own + color * (own // 2), own // 2), own // 2
                )
                source = up_own.at[pl.ds(color * (own // 2), own // 2)] if piece == 0 else up.place(
                    color, piece
                )
                return pltpu.make_async_copy(source, up_v.at[at], place_sem.at[color, piece])

            def spell():
                for d in range(n_dp):
                    for k in range(4):
                        for r in range(lines):
                            vectors[k : k + 1, pl.ds(d * own + r * 128, 128)] = p_all[
                                d, k * lines + r : k * lines + r + 1, :
                            ]
                    for r in range(unit // 128):
                        line = 9 * lines + z * (unit // 128) + r
                        vectors[4:5, pl.ds(d * unit + r * 128, 128)] = p_all[
                            d, pl.ds(line, 1), :
                        ]

            def norm(shard):
                block = 32

                def step(i, carry):
                    at = tile(i, block)
                    row = x_all[shard, at, :].astype(f32)
                    center = row - jnp.mean(row, axis=1, keepdims=True)
                    factor = lax.rsqrt(
                        jnp.mean(center * center, axis=1, keepdims=True) + epsilon
                    )
                    normed = center * factor
                    to = pl.ds(pl.multiple_of(shard * rows + i * block, block), block)
                    attn_in[to, :] = (normed * vectors[0:1, :width] + vectors[1:2, :width]).astype(
                        bf16
                    )
                    mlp_in[to, :] = (normed * vectors[2:3, :width] + vectors[3:4, :width]).astype(
                        bf16
                    )
                    return carry

                lax.fori_loop(0, rows // block, step, 0)

            def inner_tile(j):
                at = tile(j, 256)
                inner = dot(mlp_in[...], up_v[:, at], ((1,), (0,))) + vectors[4:5, at]
                cumulative = 0.5 * (1.0 + lax.erf(inner * 0.7071067811865476))
                hidden[:, at] = (inner * cumulative).astype(bf16)
                slope[:, at] = (
                    cumulative + inner * jnp.exp(-0.5 * inner * inner) * 0.3989422804014327
                )

            for color in range(2):
                placed(color, 0).start()

        def first():
            direct.receive()
            p_keep.wait()
            x_keep.wait()
            if whole:
                spell()
                norm(z)

        def x_step(k, way, step):
            step()
            if whole:
                chain = chains[0]
                pl.when(chain.has(way, k))(lambda: norm(z - k if way == 0 else z + k))

        events = [(0.3, first)]
        for i, chain in enumerate(chains):
            for at, step in enumerate(chain.steps()):
                k, way = at // 2 + 1, at % 2
                if i == 0:
                    events.append((k + 0.1, functools.partial(x_step, k, way, step)))
                else:
                    events.append((k + 0.11, step))

        def down_begin():
            loads[-1].wait()
            down.begin()
            down_keep.start()
            scatter.begin()

        events.append((0.1, down_begin))
        for i, spread in enumerate((up, down)):
            pieces = [piece for pair in zip(*spread.arrivals()) for piece in pair]
            for at, (piece, step) in enumerate(zip(pieces, spread.steps())):
                color = at % 2
                order = spread.orders[color]
                chips = piece & ~1
                time = 3 if chips.bit_count() > 1 else 1 + (chips != order[0]) if chips else 0.5

                def run(step=step, color=color, piece=piece, first=i == 0):
                    step()
                    if first and whole:
                        placed(color, piece).start()

                events.append((chips.bit_count() + 0.2 + 0.1 * i + 0.5 * (piece & 1), run))
        events.sort(key=lambda event: event[0])
        early = [event for time, event in events if time <= 3.25]
        late = [event for time, event in events if time > 3.25]
        in_turn(early)
        if whole:
            for color in range(2):
                for piece in range(n_dp):
                    placed(color, piece).wait()
            woven(late, inner_tile, units // 256)
        else:
            in_turn(late)
        for keep in (c_keep, up_keep, down_keep):
            keep.wait()
        for part in (*chains, up, down, direct, scatter):
            part.finish()

    outs = [
        jax.ShapeDtypeStruct((n_seq, rows, width), x.dtype),
        jax.ShapeDtypeStruct((n_seq, rows, width), x.dtype),
        jax.ShapeDtypeStruct((n_dp, *params.shape), params.dtype),
        jax.ShapeDtypeStruct((n_dp, own, units), w_up.dtype),
        jax.ShapeDtypeStruct((n_dp, unit, width), w_down.dtype),
        jax.ShapeDtypeStruct((owners, own // n_dp, width), w_out.dtype),
    ]
    specs = [INSIDE, ANYWHERE, INSIDE, ANYWHERE, ANYWHERE, ANYWHERE]
    scratch = [
        pltpu.VMEM((own, units), w_up.dtype),
        pltpu.VMEM((unit, width), w_down.dtype),
        pltpu.SemaphoreType.DMA((n_dp + 1,)),
        pltpu.SemaphoreType.DMA((5,)),
    ]
    if whole:
        outs += [
            jax.ShapeDtypeStruct((length, width), bf16),
            jax.ShapeDtypeStruct((length, width), bf16),
            jax.ShapeDtypeStruct((length, units), bf16),
            jax.ShapeDtypeStruct((length, units), f32),
        ]
        specs += [INSIDE] * 4
        scratch += [
            pltpu.VMEM((width, units), bf16),
            pltpu.VMEM((8, max(width, units)), f32),
            pltpu.SemaphoreType.DMA((2, n_dp)),
        ]
    return remote_call(
        0,
        body,
        outs,
        specs,
        [INSIDE] * 3 + [ANYWHERE] * 3,
        scratch
        + Chain.sems(n_seq) * 2
        + Spread.sems(n_dp) * 2
        + Direct.sems(n_dp)
        + Scatter.sems(n_dp, owners),
        (x, c, params, w_up, w_down, w_out),
    )


def maker(left, turned, right, columns):
    block = turned.shape[0]
    rows = block // 2

    def make(chip, store):
        turned[...] = left[:, tile(chip, block)].astype(jnp.float32).T.astype(turned.dtype)

        def step(j, carry):
            at = tile(j, columns)
            values = dot(turned[...], right[:, at], ((1,), (0,)))
            for core in range(2):
                store(core, at, values[core * rows : (core + 1) * rows])
            return carry

        lax.fori_loop(0, right.shape[1] // columns, step, 0)

    return make


def mixed(*lists):
    lists = [list(items) for items in lists]
    result = []
    while any(lists):
        for items in lists:
            if items:
                result.append(items.pop(0))
    return result


def down_step(n_dp, hidden, c, slope, down_w):
    f32, bf16 = jnp.float32, jnp.bfloat16
    length, units = hidden.shape
    width = c.shape[1]
    half = units // n_dp // 2

    def body(*refs):
        ins, outs, (dw, slopes, turned, load_sem), scratch = take(refs, 4, 4, 4, 100)
        h_ref, c_ref, s_ref, dw_ref = ins
        sum_ref, grad_ref, bias_ref, mlp_ref = outs
        me, z = lax.axis_index("dp"), lax.axis_index("seq")
        loads = load_all([(dw_ref, dw), (s_ref, slopes)], load_sem)
        greet(n_dp, 1, me, z)
        reduce = Reduce(
            n_dp, me, None, sum_ref, scratch, make=maker(h_ref, turned, c_ref, min(512, width))
        )

        def compute(j):
            at = tile(j, 256)
            grad = dot(c_ref[...], dw[at, :], ((1,), (1,))) * slopes[:, at]
            bias_ref[:, at] = jnp.sum(grad, axis=0, keepdims=True)
            grad_ref[:, at] = grad.astype(bf16)

        def compute_out(j):
            at = tile(j, 256)
            mlp_ref[:, at] = dot(h_ref[...], dw[:, at], ((1,), (0,)))

        turns = list(reduce.steps())
        in_turn(turns[:n_dp])
        for load in loads:
            load.wait()
        early = n_dp // 2
        woven(turns[n_dp : n_dp + early], compute, units // 256, first=units // 512)
        woven(turns[n_dp + early :], compute_out, width // 256, first=width // 512)
        reduce.finish()

    return remote_call(
        1,
        body,
        [
            jax.ShapeDtypeStruct((units // n_dp, width), bf16),
            jax.ShapeDtypeStruct((length, units), bf16),
            jax.ShapeDtypeStruct((1, units), f32),
            jax.ShapeDtypeStruct((length, width), f32),
        ],
        [INSIDE] * 4,
        [INSIDE] * 2 + [ANYWHERE] * 2,
        [
            pltpu.VMEM((units, width), bf16),
            pltpu.VMEM((length, units), f32),
            pltpu.VMEM((4 * half, length), bf16),
            pltpu.SemaphoreType.DMA((2,)),
        ]
        + Reduce.scratch(n_dp, half, width, bf16, made=True),
        (hidden, c, slope, down_w),
    )


def up_step(n_dp, n_seq, left, right, weights, out_own, w_qkv):
    f32, bf16 = jnp.float32, jnp.bfloat16
    length, rows = left.shape
    cols = right.shape[1]
    half = rows // n_dp // 2
    own = w_qkv.shape[0]
    part = H // n_seq * HD

    def body(*refs):
        ins, outs, own_scratch, sems, sems_qkv, scratch = take(refs, 5, 4, 5, 2, 2, 100)
        l_ref, r_ref, w_ref, out_ref, qkv_ref = ins
        sum_ref, back_ref, out_all, qkv_all = outs
        w, turned, qkv_own, load_sem, keep_sem = own_scratch
        me, z = lax.axis_index("dp"), lax.axis_index("seq")
        loads = load_all(
            [(w_ref, w)]
            + [
                (
                    qkv_ref.at[:, pl.ds(pl.multiple_of(i * H * HD + z * part, HD), part)],
                    qkv_own.at[:, pl.ds(i * part, part)],
                )
                for i in range(3)
            ],
            load_sem,
        )
        greet(n_dp, 1, me, z)
        reduce = Reduce(
            n_dp, me, None, sum_ref, scratch, make=maker(l_ref, turned, r_ref, min(512, cols))
        )
        out = Spread(n_dp, me, out_ref, out_all, sems)
        qkv = Spread(n_dp, me, qkv_own, qkv_all, sems_qkv)
        keep = pltpu.make_async_copy(out_ref, out_all.at[me], keep_sem.at[0])
        keep_qkv = pltpu.make_async_copy(qkv_own, qkv_all.at[me], keep_sem.at[1])

        def compute(j):
            at = tile(j, 256)
            back_ref[:, at] = dot(r_ref[...], w[at, :], ((1,), (1,)))

        for load in loads[1:]:
            load.wait()
        qkv.begin()
        out.begin()
        keep_qkv.start()
        keep.start()
        turns = list(reduce.steps())
        in_turn(turns[:n_dp])
        loads[0].wait()
        woven(mixed(turns[n_dp:], qkv.steps(), out.steps()), compute, rows // 256)
        keep_qkv.wait()
        keep.wait()
        for one in (reduce, qkv, out):
            one.finish()

    return remote_call(
        2,
        body,
        [
            jax.ShapeDtypeStruct((rows // n_dp, cols), bf16),
            jax.ShapeDtypeStruct((length, rows), f32),
            jax.ShapeDtypeStruct((n_dp, *out_own.shape), bf16),
            jax.ShapeDtypeStruct((n_dp, own, 3 * part), bf16),
        ],
        [INSIDE] * 2 + [ANYWHERE] * 2,
        [INSIDE] * 2 + [ANYWHERE, INSIDE, ANYWHERE],
        [
            pltpu.VMEM((rows, cols), bf16),
            pltpu.VMEM((4 * half, length), bf16),
            pltpu.VMEM((own, 3 * part), bf16),
            pltpu.SemaphoreType.DMA((4,)),
            pltpu.SemaphoreType.DMA((2,)),
        ]
        + Spread.sems(n_dp) * 2
        + Reduce.scratch(n_dp, half, cols, bf16, made=True),
        (left, right, weights, out_own, w_qkv),
    )


def attention_step(n_dp, left, right, weights):
    f32, bf16 = jnp.float32, jnp.bfloat16
    length, rows = left.shape
    cols = right.shape[1]
    half = rows // n_dp // 2
    own = rows // n_dp
    size = 2 + 3 + 3 * (bits_of(n_dp) - 1)

    def body(*refs):
        ins, outs, (w, turned, load_sem), second = take(refs, 3, 2, 3, size)
        l_ref, r_ref, w_ref = ins
        sum_ref, back_ref = outs
        me, z = lax.axis_index("dp"), lax.axis_index("seq")
        loads = load_all([(w_ref, w)], load_sem)
        greet(n_dp, 1, me, z)
        reduce = Reduce(
            n_dp, me, None, sum_ref, second, make=maker(l_ref, turned, r_ref, min(512, cols))
        )

        def compute(j):
            at = tile(j, 256)
            back_ref[:, at] = dot(r_ref[...], w[at, :], ((1,), (1,)))

        turns = list(reduce.steps())
        in_turn(turns[:n_dp])
        loads[0].wait()
        woven(turns[n_dp:], compute, rows // 256)
        reduce.finish()

    return remote_call(
        3,
        body,
        [
            jax.ShapeDtypeStruct((own, cols), bf16),
            jax.ShapeDtypeStruct((length, rows), f32),
        ],
        [INSIDE] * 2,
        [INSIDE] * 2 + [ANYWHERE],
        [
            pltpu.VMEM((rows, cols), bf16),
            pltpu.VMEM((4 * half, length), bf16),
            pltpu.SemaphoreType.DMA((1,)),
        ]
        + Reduce.scratch(n_dp, half, cols, bf16, made=True),
        (left, right, weights),
    )


def attend(attn_in, triple_w, triple_b, out_w, c, mlp_out, cosine, sine):
    f32, bf16 = jnp.float32, jnp.bfloat16
    length, width = attn_in.shape
    part = triple_w.shape[1] // 3
    heads = part // HD
    scale = HD ** (-0.5)

    def body(a_ref, tb_ref, cos_ref, sin_ref, c_ref, ow_hbm, tw_hbm, mlp_hbm, *rest):
        grad_ref, bias_ref, merged_ref, ahead_ref, tw, ow_ref, mlp, triple, sems = rest
        n_dp, owners, piece, _ = ow_hbm.shape
        loads = load_all(
            [(tw_hbm, tw), (mlp_hbm, mlp)]
            + [
                (
                    ow_hbm.at[d, slot],
                    ow_ref.at[pl.ds((slot * n_dp + d) * piece, piece)],
                )
                for d in range(n_dp)
                for slot in range(owners)
            ],
            sems,
        )
        lanes = lax.broadcasted_iota(jnp.int32, (length, 128), 1)

        def turned(values, direction):
            head = values[:, :128]
            swapped = jnp.where(
                lanes < ROT // 2,
                pltpu.roll(head, 128 - ROT // 2, 1),
                pltpu.roll(head, ROT // 2, 1),
            )
            head = head * cos_ref[...] + direction * swapped * sin_ref[...]
            return jnp.concatenate([head, values[:, 128:]], axis=1)

        rows = lax.broadcasted_iota(jnp.int32, (length, length), 0)
        cols = lax.broadcasted_iota(jnp.int32, (length, length), 1)
        loads[0].wait()

        def project(j, carry):
            at = tile(j, HD)
            triple[:, at] = dot(a_ref[...], tw[:, at], ((1,), (0,))) + tb_ref[:, at]
            return carry

        lax.fori_loop(0, 3 * heads, project, 0)
        for load in loads[2:]:
            load.wait()

        def head(h, carry):
            at = [tile(i * heads + h, HD) for i in range(3)]
            q = turned(triple[:, at[0]], 1.0).astype(bf16)
            k = turned(triple[:, at[1]], 1.0).astype(bf16)
            v = triple[:, at[2]].astype(bf16)
            scores = jnp.where(cols <= rows, dot(q, k, ((1,), (1,))) * scale, masked_fill)
            top = jnp.max(scores, axis=1, keepdims=True)
            logsum = top + jnp.log(jnp.sum(jnp.exp(scores - top), axis=1, keepdims=True))
            probs_f = jnp.exp(scores - logsum)
            probs = probs_f.astype(bf16)
            context = dot(probs, v, ((1,), (0,))).astype(bf16)
            merged_ref[:, at[0]] = context
            context_grad = dot(c_ref[...], ow_ref[at[0], :], ((1,), (1,))).astype(bf16)
            delta = jnp.sum(context_grad.astype(f32) * context.astype(f32), axis=1, keepdims=True)
            prob_grad = dot(context_grad, v, ((1,), (1,)))
            score_grad = probs_f * (prob_grad - delta) * scale
            score_grad_b = score_grad.astype(bf16)
            query_grad = dot(score_grad_b, k, ((1,), (0,))).astype(bf16).astype(f32)
            key_grad = (
                dot(score_grad_b.astype(f32).T.astype(bf16), q, ((1,), (0,)))
                .astype(bf16)
                .astype(f32)
            )
            value_grad = (
                dot(probs.astype(f32).T.astype(bf16), context_grad, ((1,), (0,)))
                .astype(bf16)
                .astype(f32)
            )
            for where, grad in zip(
                at, (turned(query_grad, -1.0), turned(key_grad, -1.0), value_grad)
            ):
                grad_ref[:, where] = grad.astype(bf16)
                bias_ref[:, where] = jnp.sum(grad, axis=0, keepdims=True)
            return carry

        lax.fori_loop(0, heads, head, 0)
        loads[1].wait()

        def join(j, carry):
            at = tile(j, 256)
            total = dot(merged_ref[...], ow_ref[:, at], ((1,), (0,))) + mlp[:, at]
            ahead_ref[:, at] = total.astype(bf16)
            return carry

        lax.fori_loop(0, width // 256, join, 0)

    return pl.pallas_call(
        body,
        out_shape=(
            jax.ShapeDtypeStruct((length, 3 * part), bf16),
            jax.ShapeDtypeStruct((1, 3 * part), f32),
            jax.ShapeDtypeStruct((length, part), bf16),
            jax.ShapeDtypeStruct((length, width), bf16),
        ),
        in_specs=[INSIDE] * 5 + [ANYWHERE] * 3,
        out_specs=(INSIDE,) * 4,
        scratch_shapes=[
            pltpu.VMEM((width, 3 * part), bf16),
            pltpu.VMEM((part, width), bf16),
            pltpu.VMEM((length, width), f32),
            pltpu.VMEM((length, 3 * part), f32),
            pltpu.SemaphoreType.DMA((2 + out_w.shape[0] * out_w.shape[1],)),
        ],
        cost_estimate=pl.CostEstimate(
            flops=20_000_000_000, bytes_accessed=30_000_000, transcendentals=0
        ),
        name="attend",
    )(attn_in, triple_b, cosine, sine, c, out_w, triple_w, mlp_out)


def last_step(n_dp, n_seq, qkv_sum, out_grad, small, ahead, back):
    f32, bf16 = jnp.float32, jnp.bfloat16
    rows, width = back.shape[0] // n_seq, back.shape[1]
    owners = n_dp // n_seq
    few = small.shape[0] // n_dp
    pieces = 4
    size = 2 + 3 + 3 * (bits_of(n_dp) - 1)

    def body(*refs):
        ins, outs, (small_sum, keep_sem), sq, so, ss, a, b, scratch, first = take(
            refs, 5, 6, 2, 2, 2, 2, 4, 4, size, size
        )
        q_ref, g_ref, s_ref, a_ref, b_ref = ins
        q_out, o_out, s_out, a_out, b_out, out_sum = outs
        me, z = lax.axis_index("dp"), lax.axis_index("seq")
        greet(n_dp, n_seq, me, z)
        chain = Chain(n_seq, z, q_ref, q_out, sq)
        little = Reduce(n_dp, me, s_ref, small_sum, scratch)
        tiny = Chain(n_seq, z, small_sum, s_out, ss)
        one = Settle(n_seq, z, a_ref, a_out, a)
        two = Settle(n_seq, z, b_ref, b_out, b)
        cast = Cast(n_seq, z, me // owners, out_sum, o_out, so, pieces)
        out = Reduce(
            n_dp,
            me,
            g_ref,
            out_sum,
            first,
            rows_at=lambda dest: 2 * (dest % owners),
            held_by=lambda dest: dest // owners == z,
        )
        chain.begin()
        keep = pltpu.make_async_copy(q_ref, q_out.at[z], keep_sem.at[0])
        keep.start()
        little.begin()
        out.begin()
        turns = list(out.steps())
        meets = n_dp // 2
        in_turn(mixed(little.steps(), turns[:meets]))
        tiny.begin()
        keep_small = pltpu.make_async_copy(small_sum, s_out.at[z], keep_sem.at[1])
        keep_small.start()
        one.begin()

        events = [(4.4, cast.begin), (4.45, two.begin)]
        merges = turns[meets:]
        for at, step in enumerate(merges):
            events.append((1.4 + 2.4 * at / len(merges), step))
        for at, step in enumerate(chain.steps()):
            events.append((1.5 * (at // 2 + 1), step))
        for at, step in enumerate(tiny.steps()):
            events.append((1.5 * (at // 2 + 1) + 0.1, step))
        for start, settle in ((2.4, one), (7.4, two)):
            steps = list(settle.steps())
            for at, step in enumerate(steps[:-3]):
                events.append((start + at // 2, step))
            events.append((start - 2, steps[-3]))
            for step in steps[-2:]:
                events.append((start + n_seq - 2, step))
        for at, step in enumerate(cast.steps()):
            events.append((5.6 + 0.5 * (at // 2), step))
        in_turn([step for _, step in sorted(events, key=lambda event: event[0])])
        keep.wait()
        keep_small.wait()
        for part in (chain, tiny, one, two, cast, little, out):
            part.finish()

    return remote_call(
        4,
        body,
        [
            jax.ShapeDtypeStruct((n_seq, *qkv_sum.shape), bf16),
            jax.ShapeDtypeStruct((width // n_dp, width), bf16),
            jax.ShapeDtypeStruct((n_seq, few, small.shape[1]), f32),
            jax.ShapeDtypeStruct((rows, width), f32),
            jax.ShapeDtypeStruct((rows, width), f32),
            jax.ShapeDtypeStruct((width // n_dp, width), bf16),
        ],
        [ANYWHERE] * 3 + [INSIDE] * 3,
        [INSIDE] + [ANYWHERE] * 2 + [INSIDE] * 2,
        [pltpu.VMEM((few, small.shape[1]), f32), pltpu.SemaphoreType.DMA((2,))]
        + Chain.sems(n_seq)
        + Cast.sems(pieces)
        + Chain.sems(n_seq)
        + Settle.scratch(n_seq, rows, width, bf16) * 2
        + Reduce.scratch(n_dp, few // 2, small.shape[1], f32)
        + Reduce.scratch(n_dp, width // n_dp // 2, width, bf16),
        (
            qkv_sum,
            out_grad,
            small,
            ahead.reshape(n_seq, rows, width),
            back.reshape(n_seq, rows, width),
        ),
    )


def widen_kernel(parts_ref, out_ref):
    count, _, unit = parts_ref.shape
    for s in range(count):
        out_ref[:, s * unit : (s + 1) * unit] = parts_ref[s].astype(jnp.float32)


def widen(parts, blocks):
    n_seq, rows, cols = parts.shape
    unit = cols // blocks
    if unit % 128:
        return (
            parts.reshape(n_seq, rows, blocks, unit)
            .transpose(1, 2, 0, 3)
            .reshape(rows, n_seq * cols)
            .astype(jnp.float32)
        )
    return pl.pallas_call(
        widen_kernel,
        grid=(blocks,),
        out_shape=jax.ShapeDtypeStruct((rows, n_seq * cols), jnp.float32),
        in_specs=[pl.BlockSpec((n_seq, rows, unit), lambda j: (0, 0, j))],
        out_specs=pl.BlockSpec((rows, n_seq * unit), lambda j: (0, j)),
        cost_estimate=pl.CostEstimate(
            flops=0, bytes_accessed=6 * n_seq * rows * cols, transcendentals=0
        ),
        name="widen",
    )(parts)


def held(after, *values):
    return lax.optimization_barrier((*values, after))[:-1]


def normalize(rows):
    center = rows - jnp.mean(rows, axis=-1, keepdims=True)
    factor = lax.rsqrt(jnp.mean(center * center, axis=-1, keepdims=True) + epsilon)
    return center * factor, factor


def angles(positions):
    half = ROT // 2
    freqs = 10000.0 ** (-2.0 * jnp.arange(half).astype(positions.dtype) / ROT)
    theta = positions[:, None] * freqs[None, :]
    return (jnp.cos(theta), jnp.sin(theta))


def gather_seq(shard):
    return lax.all_gather(shard, "seq", axis=0, tiled=False)


def make_local(n_dp, n_seq):
    def local(
        layer_input,
        cotangent,
        ln1_gain,
        ln1_bias,
        w_qkv,
        b_qkv,
        w_out,
        b_out,
        ln2_gain,
        ln2_bias,
        w_up,
        b_up,
        w_down,
        b_down,
    ):
        f32, bf16 = jnp.float32, jnp.bfloat16
        _, tok_local, width = layer_input.shape
        length = tok_local * n_seq
        own = width // n_dp
        ff = w_up.shape[1]
        ff_own = ff // n_dp
        unit = ff_own // n_seq
        heads = H // n_seq
        owners = n_dp // n_seq
        z = lax.axis_index("seq")
        me = lax.axis_index("dp")

        packed = jnp.concatenate(
            [ln1_gain, ln1_bias, ln2_gain, ln2_bias, b_out, b_down, b_qkv, b_up]
        )
        packed = jnp.pad(packed, (0, -packed.shape[0] % 2048)).reshape(-1, 128)
        tokens, incoming, gathered, up_w, down_w, out_own, *made = fetch(
            n_dp,
            n_seq,
            unit,
            layer_input.reshape(tok_local, width),
            cotangent.reshape(tok_local, width),
            packed,
            w_up,
            w_down,
            w_out,
        )
        tokens, incoming = tokens.reshape(length, width), incoming.reshape(length, width)
        gathered = gathered.reshape(n_dp, -1)
        up_w = up_w.reshape(width, n_dp * unit)
        down_w = down_w.reshape(n_dp * unit, width)

        gain_one, shift_one, gain_two, shift_two, out_b, down_b = (
            gathered[:, k * own : (k + 1) * own].reshape(width) for k in range(6)
        )
        base = 6 * own
        triple_b = lax.dynamic_slice_in_dim(
            gathered[:, base : base + 3 * own].reshape(3, H, HD), z * heads, heads, 1
        ).reshape(3 * heads * HD)
        up_b = lax.dynamic_index_in_dim(
            gathered[:, base + 3 * own : base + 3 * own + ff_own].reshape(n_dp, n_seq, unit),
            z,
            1,
            keepdims=False,
        ).reshape(n_dp * unit)

        if made:
            mlp_in, attn_in, hidden, slope = made
        else:
            normed, _ = normalize(tokens.astype(f32))
            mlp_in = (normed * gain_two + shift_two).astype(bf16)
            attn_in = (normed * gain_one + shift_one).astype(bf16)
            inner = dot(mlp_in, up_w, ((1,), (0,))) + up_b
            cumulative = 0.5 * (1.0 + lax.erf(inner * 0.7071067811865476))
            hidden = (inner * cumulative).astype(bf16)
            slope = cumulative + inner * jnp.exp(-0.5 * inner * inner) * 0.3989422804014327
        down_sum, inner_grad_b, b_up_grad, mlp_out = down_step(
            n_dp, hidden, incoming, slope, down_w
        )
        down_part = gather_seq(down_sum)
        up_sum, mlp_in_grad, out_w, triple_w = up_step(
            n_dp,
            n_seq,
            mlp_in,
            inner_grad_b,
            up_w,
            out_own.reshape(-1, width),
            w_qkv,
        )
        up_part = gather_seq(up_sum)
        out_w = out_w.reshape(n_dp, owners, own // n_dp, width)
        triple_w = triple_w.reshape(width, 3 * heads * HD)

        (tokens,) = held(up_sum, tokens)
        normed, _ = normalize(tokens.astype(f32))
        ln2_gain_grad = jnp.sum(mlp_in_grad * normed, axis=0)
        ln2_bias_grad = jnp.sum(mlp_in_grad, axis=0)
        cosine, sine = angles(jnp.arange(length, dtype=jnp.int32).astype(f32))
        still = jnp.zeros((length, 128 - ROT), f32)
        triple_grad_b, b_qkv_grad, merged, ahead = attend(
            attn_in,
            triple_w,
            triple_b.reshape(1, -1),
            out_w,
            incoming,
            mlp_out,
            jnp.concatenate([cosine, cosine, still + 1.0], axis=1),
            jnp.concatenate([-sine, sine, still], axis=1),
        )
        out_grad = dot(merged, incoming, ((0,), (0,))).astype(bf16)
        qkv_sum, attn_in_grad = attention_step(n_dp, attn_in, triple_grad_b, triple_w)
        ln1_gain_grad = jnp.sum(attn_in_grad * normed, axis=0)
        ln1_bias_grad = jnp.sum(attn_in_grad, axis=0)

        rows = layer_input.reshape(tok_local, width).astype(f32)
        grad_rows = cotangent.reshape(tok_local, width).astype(f32)
        here = jnp.arange(n_seq) == z
        b_up_wide = jnp.where(
            here[None, :, None], b_up_grad.reshape(n_dp, 1, unit), 0.0
        ).reshape(n_dp, ff_own)
        b_qkv_wide = jnp.where(
            here[None, :, None], b_qkv_grad.reshape(3, 1, heads * HD), 0.0
        ).reshape(n_dp, 3 * own)
        b_down_grad = jnp.sum(grad_rows, axis=0)
        small = jnp.concatenate(
            [
                ln1_gain_grad.reshape(n_dp, own),
                ln1_bias_grad.reshape(n_dp, own),
                ln2_gain_grad.reshape(n_dp, own),
                ln2_bias_grad.reshape(n_dp, own),
                b_down_grad.reshape(n_dp, own),
                b_qkv_wide,
                b_up_wide,
            ],
            axis=1,
        )
        small_len = small.shape[1]
        small = jnp.pad(small, ((0, 0), (0, -small_len % 4096))).reshape(-1, 256)

        back = attn_in_grad * gain_one + mlp_in_grad * gain_two
        down_full = down_part.reshape(ff_own, width).astype(f32)
        (small,) = held(down_full, small)
        qkv_part, out_cast, small_all, ahead, scaled, out_sum = last_step(
            n_dp, n_seq, qkv_sum, out_grad, small, ahead, back.astype(bf16)
        )
        output = rows + (out_b + down_b) + ahead
        normed_own, factor_own = normalize(rows)
        input_grad = grad_rows + factor_own * (
            scaled
            - jnp.mean(scaled, axis=-1, keepdims=True)
            - normed_own * jnp.mean(scaled * normed_own, axis=-1, keepdims=True)
        )
        mine = jnp.sum(small_all, axis=0).reshape(-1)
        g1, s1, g2, s2, bd = (mine[k * own : (k + 1) * own] for k in range(5))
        bq = mine[5 * own : 8 * own]
        bu = mine[8 * own : small_len]
        out_full = jnp.where(me // owners == z, out_sum, out_cast).astype(f32)
        up_full = widen(up_part, n_dp)
        qkv_full = widen(qkv_part, 3)

        return (
            output.reshape(layer_input.shape),
            input_grad.reshape(layer_input.shape),
            g1,
            s1,
            qkv_full,
            bq,
            out_full,
            bd,
            g2,
            s2,
            up_full,
            bu,
            down_full,
            bd,
        )

    return local


def solution(mesh):
    vector, matrix, tokens = P("dp"), P("dp", None), P("dp", "seq", None)
    specs = (
        tokens,
        tokens,
        vector,
        vector,
        matrix,
        vector,
        matrix,
        vector,
        vector,
        vector,
        matrix,
        vector,
        matrix,
        vector,
    )
    local = make_local(mesh.shape["dp"], mesh.shape["seq"])

    return jax.shard_map(local, mesh=mesh, in_specs=specs, out_specs=specs, check_vma=False)
```
